32 devices in a mesh: band: 4 (over z), space: 8 (over y, x, core).
Axes of the slice: x: 2, y: 2, z: 4, core: 2. Of those that a mesh axis runs over, the one named last changes fastest.
Arguments:
- orbitals: float32 [2, 16, 96, 9216], P(None, 'band', 'space'), may hold values from -6 to 6
- potential: float32 [96, 9216], P('space'), may hold values from -2 to 4
- occupations: float32 [16], P('band'), may hold values from 0.5 to 2
Outputs:
- propagated: float32 [2, 16, 96, 9216], P(None, 'band', 'space')
- density: float32 [96, 9216], P('space')
- hartree: float32 [96, 9216], P('space')
The draws below stay inside these ranges and needn't reach their ends.
All inputs are finite; a program needn't handle non-finite values.
Results may differ from the reference program's by a relative error of at most 0.0029.
Values may be sent and summed in bfloat16 or wider, within the bound.
No kernel may reach another device: no remote copies, remote signals or barrier semaphores. Data moves between devices by JAX's collectives and lax.ppermute only.
A program may use at most 64 MiB of HBM per device.

```python
import math
from functools import partial
import jax
import jax.numpy as jnp
from jax import lax

NX = 96
NY = 96
NZ = 96
ORBITALS = 16


def draw_orbitals(key, part):
    shape = (2, ORBITALS, NX, NY * NZ)
    values = jax.random.normal(jax.random.fold_in(key, 11), shape, jnp.float32)
    return jnp.clip(values, -6.0, 6.0)


def draw_potential(key, part):
    shape = (NX, NY * NZ)
    return jax.random.uniform(jax.random.fold_in(key, 43), shape, jnp.float32, -2.0, 4.0)


def block_levels(own_key, dims, cuts, least, largest):
    def one(position, parts):
        draws = jax.random.uniform(jax.random.fold_in(jax.random.fold_in(own_key, 6), position), (parts,), jnp.float32, least / len(cuts), largest / len(cuts))
        return jnp.repeat(jnp.exp(draws), dims[position] // parts).reshape((-1,) + (1,) * (len(dims) - position - 1))

    factor_of = one(*cuts[0])
    for cut in cuts[1:]:
        factor_of = factor_of * one(*cut)
    return factor_of


def setup_inputs(seed: int = 0) -> dict:
    streams_of = jax.random.split(jax.random.key(seed), 4)
    orbitals = draw_orbitals(jax.random.fold_in(streams_of[3], 71), 0)
    potential = draw_potential(jax.random.fold_in(streams_of[3], 71), 0)
    occupations = jnp.clip(jnp.exp(math.log(2.0) - 1.3862944 * jax.random.uniform(streams_of[2], (ORBITALS,), jnp.float32) ** block_levels(streams_of[2], (ORBITALS,), ((0, 4),), -0.2, 0.2)), 0.5, 2.0)
    return {"orbitals": orbitals, "potential": potential, "occupations": occupations}


stencil_coeffs = (-205.0 / 72.0, 8.0 / 5.0, -1.0 / 5.0, 8.0 / 315.0, -1.0 / 560.0)
energy_shift = 6.0
energy_scale = 8.0
bessel_terms = (0.7651976865579666, 0.44005058574493355, 0.11490348493190049)


def neighbour(padded, dimension, offset, reach_cells, shape):
    starts = [0, reach_cells, reach_cells, reach_cells]
    starts[dimension] = starts[dimension] + offset
    limits = [opening + extent for opening, extent in zip(starts, shape)]
    return lax.slice(padded, starts, limits)


def scaled_operator(center, grid_potential):
    reach_cells = len(stencil_coeffs) - 1
    rounded = lax.optimization_barrier(center.astype(jnp.bfloat16)).astype(jnp.float32)
    widths = ((0, 0), (reach_cells, reach_cells), (reach_cells, reach_cells), (reach_cells, reach_cells))
    padded = jnp.pad(rounded, widths)
    summed = (3.0 * stencil_coeffs[0]) * center
    for offset in range(1, reach_cells + 1):
        for dimension in (1, 2, 3):
            after = neighbour(padded, dimension, offset, reach_cells, center.shape)
            before = neighbour(padded, dimension, -offset, reach_cells, center.shape)
            summed = summed + stencil_coeffs[offset] * (after + before)
    energy = -0.5 * summed + grid_potential * center
    return (energy - energy_shift * center) / energy_scale


def propagate_one(orbital_pair, grid_potential):
    start = orbital_pair.reshape(2, NX, NY, NZ)
    first = scaled_operator(start, grid_potential)
    second = 2.0 * scaled_operator(first, grid_potential) - start
    real_out = bessel_terms[0] * start[0] + 2.0 * bessel_terms[1] * first[1] - 2.0 * bessel_terms[2] * second[0]
    imag_out = bessel_terms[0] * start[1] - 2.0 * bessel_terms[1] * first[0] - 2.0 * bessel_terms[2] * second[1]
    return jnp.stack([real_out, imag_out]).reshape(2, NX, NY * NZ)


def squared_waves(length):
    indices = lax.iota(jnp.int32, length)
    signed = jnp.where(indices < (length + 1) // 2, indices, indices - length).astype(jnp.float32)
    return (2.0 * math.pi / length * signed) ** 2


def reference(orbitals, potential, occupations):
    grid_potential = potential.reshape(NX, NY, NZ)
    moved = jnp.moveaxis(orbitals, 1, 0)
    results = lax.map(partial(propagate_one, grid_potential=grid_potential), moved)
    propagated = jnp.moveaxis(results, 0, 1)
    weights = occupations / ORBITALS
    density = jnp.sum(weights[:, None, None] * (propagated[0] * propagated[0] + propagated[1] * propagated[1]), axis=0)
    squares = squared_waves(NX)[:, None, None] + squared_waves(NY)[None, :, None] + squared_waves(NZ)[None, None, :]
    kernel = jnp.where(squares > 0, 4.0 * math.pi / jnp.where(squares > 0, squares, 1.0), 0.0)
    spectral = jnp.fft.fftn(density.reshape(NX, NY, NZ))
    hartree = jnp.real(jnp.fft.ifftn(spectral * kernel)).reshape(NX, NY * NZ).astype(jnp.float32)
    return propagated, density, hartree
```

```python
import math

import jax
import jax.numpy as jnp
import numpy as np
from jax import lax
from jax.experimental import pallas as pl
from jax.experimental.pallas import tpu as pltpu
from jax.sharding import PartitionSpec as P

NX = 96
NY = 96
NZ = 96


stencil_coeffs = (-205.0 / 72.0, 8.0 / 5.0, -1.0 / 5.0, 8.0 / 315.0, -1.0 / 560.0)
energy_shift = 6.0
energy_scale = 8.0
bessel_terms = (0.7651976865579666, 0.44005058574493355, 0.11490348493190049)


def from_behind(x, axis, by):
    count = lax.axis_size(axis)
    pairs = [(i, i + by) for i in range(count) if 0 <= i + by < count]
    return lax.ppermute(x, axis, pairs)


def plane_laplace(center, wider):
    reach_cells = len(stencil_coeffs) - 1
    planes = center.shape[-2]
    cells = center.shape[-1]
    spread = wider.astype(jnp.float32)
    middle = spread[..., reach_cells : reach_cells + planes, :]
    summed = 3.0 * stencil_coeffs[0] * center
    for offset in range(1, reach_cells + 1):
        after = spread[..., reach_cells + offset : reach_cells + offset + planes, :]
        before = spread[..., reach_cells - offset : reach_cells - offset + planes, :]
        summed = summed + stencil_coeffs[offset] * (after + before)
    margin = reach_cells * NZ
    padded = jnp.pad(middle, [(0, 0)] * (middle.ndim - 1) + [(margin, margin)])
    z_index = lax.iota(jnp.int32, cells) % NZ
    for offset in range(1, reach_cells + 1):
        stride = offset * NZ
        beyond = padded[..., margin + stride : margin + stride + cells]
        behind = padded[..., margin - stride : margin - stride + cells]
        summed = summed + stencil_coeffs[offset] * (beyond + behind)
        beyond = jnp.where(
            z_index + offset < NZ, padded[..., margin + offset : margin + offset + cells], 0.0
        )
        behind = jnp.where(
            z_index - offset >= 0, padded[..., margin - offset : margin - offset + cells], 0.0
        )
        summed = summed + stencil_coeffs[offset] * (beyond + behind)
    return summed


def scaled_hamiltonian(center, wider, field_values):
    energy = -0.5 * plane_laplace(center, wider) + field_values * center
    return (energy - energy_shift * center) / energy_scale


def slab_rims(source, extent):
    planes = source.shape[-2]
    lower_parts = []
    upper_parts = []
    for distance in range(1, -(-extent // planes) + 1):
        needed = min(planes, extent - (distance - 1) * planes)
        for heading in (1, -1):
            if heading == 1:
                outgoing = source[..., planes - needed :, :]
            else:
                outgoing = source[..., :needed, :]
            arrived = from_behind(outgoing, "space", heading * distance)
            if heading == 1:
                lower_parts.append(arrived)
            else:
                upper_parts.append(arrived)
    return jnp.concatenate(lower_parts[::-1] + [source] + upper_parts, axis=-2)


def dft_tables(length):
    indices = lax.iota(jnp.int32, length)
    product = indices[:, None] * indices[None, :] % length
    phases = 2.0 * math.pi / length * product.astype(jnp.float32)
    return (jnp.cos(phases), jnp.sin(phases))


def turn_axis(cosine, sines, values, pattern):
    direct = jnp.einsum(pattern, cosine, values, precision=lax.Precision.HIGHEST)
    crossed = jnp.einsum(pattern, sines, values, precision=lax.Precision.HIGHEST)
    real_part = direct[..., :NZ] - crossed[..., NZ:]
    imag_part = direct[..., NZ:] + crossed[..., :NZ]
    return jnp.concatenate([real_part, imag_part], axis=-1)


def squared_waves(length, anchor, extent):
    indices = anchor + lax.iota(jnp.int32, extent)
    signed = jnp.where(indices < (length + 1) // 2, indices, indices - length).astype(jnp.float32)
    return (2.0 * math.pi / length * signed) ** 2


def hartree_field(density):
    planes = density.shape[0]
    z_cosine, z_sine = dft_tables(NZ)
    y_cosine, y_sine = dft_tables(NY)
    x_cosine, x_sine = dft_tables(NX)
    forward_z = jnp.concatenate([z_cosine, -z_sine], axis=1)
    flattened = density.reshape(planes * NY, NZ)
    spectral = jnp.dot(
        flattened, forward_z, precision=lax.Precision.HIGHEST, preferred_element_type=jnp.float32
    )
    spectral = turn_axis(y_cosine, -y_sine, spectral.reshape(planes, NY, 2 * NZ), "ky,xyz->xkz")
    columns = lax.all_to_all(spectral, "space", split_axis=1, concat_axis=0, tiled=True)
    y_rows = columns.shape[1]
    spectral = turn_axis(x_cosine, -x_sine, columns, "kx,xyz->kyz")
    squares = (
        squared_waves(NX, 0, NX)[:, None, None]
        + squared_waves(NY, lax.axis_index("space") * y_rows, y_rows)[None, :, None]
        + squared_waves(NZ, 0, NZ)[None, None, :]
    )
    kernel = jnp.where(squares > 0, 4.0 * math.pi / jnp.where(squares > 0, squares, 1.0), 0.0)
    spectral = spectral * jnp.concatenate([kernel, kernel], axis=-1)
    spectral = turn_axis(x_cosine, x_sine, spectral, "kx,xyz->kyz")
    slabs = lax.all_to_all(spectral, "space", split_axis=0, concat_axis=1, tiled=True)
    spectral = turn_axis(y_cosine, y_sine, slabs, "ky,xyz->xkz")
    inverse_z = jnp.concatenate([z_cosine, -z_sine], axis=0)
    field_values = jnp.dot(
        spectral.reshape(planes * NY, 2 * NZ),
        inverse_z,
        precision=lax.Precision.HIGHEST,
        preferred_element_type=jnp.float32,
    )
    return (field_values / (NX * NY * NZ)).reshape(planes, NY * NZ)


def per_device_general(orbitals, potential, occupations):
    reach_cells = len(stencil_coeffs) - 1
    orbital_count = orbitals.shape[1]
    zero_copy = slab_rims(orbitals.astype(jnp.bfloat16), reach_cells)
    first_term = scaled_hamiltonian(orbitals, zero_copy, potential)
    first_copy = slab_rims(first_term.astype(jnp.bfloat16), reach_cells)
    second_term = 2.0 * scaled_hamiltonian(first_term, first_copy, potential) - orbitals
    prop_real = (
        bessel_terms[0] * orbitals[0]
        + 2.0 * bessel_terms[1] * first_term[1]
        - 2.0 * bessel_terms[2] * second_term[0]
    )
    prop_imag = (
        bessel_terms[0] * orbitals[1]
        - 2.0 * bessel_terms[1] * first_term[0]
        - 2.0 * bessel_terms[2] * second_term[1]
    )
    propagated = jnp.stack([prop_real, prop_imag])
    weights = occupations / (orbital_count * lax.axis_size("band"))
    partial_density = jnp.sum(
        weights[:, None, None] * (prop_real * prop_real + prop_imag * prop_imag), axis=0
    )
    density = lax.psum(partial_density, "band")
    hartree = hartree_field(density)
    return (propagated, density, hartree)


REACH = len(stencil_coeffs) - 1
TABLE_SCALE = 5040.0
CHUNK = 768
WINDOW = 1024
TILE = 256
MARGIN = 384


def plane_table():
    phases = CHUNK // TILE
    table = np.zeros((phases, WINDOW, TILE), np.float32)
    scaled = [round(coeff * TABLE_SCALE) for coeff in stencil_coeffs[1:]]
    for phase in range(phases):
        target = phase * TILE + np.arange(TILE)[None, :]
        origin = phase * TILE - MARGIN + np.arange(WINDOW)[:, None]
        y_step = origin // NZ - target // NZ
        z_step = origin % NZ - target % NZ
        for offset in range(1, REACH + 1):
            along_y = (np.abs(y_step) == offset) & (z_step == 0)
            along_z = (y_step == 0) & (np.abs(z_step) == offset)
            table[phase] += scaled[offset - 1] * (along_y | along_z)
    return jnp.asarray(table, jnp.bfloat16)


def joined(block, plane, lanes=slice(None)):
    return jnp.concatenate([block[0, plane, :, lanes], block[1, plane, :, lanes]], axis=0)


def rim_kernel(orbitals, lower, upper):
    step = pl.program_id(0)
    value = joined(orbitals, 0).astype(jnp.bfloat16)

    @pl.when(step < REACH)
    def _():
        lower[0] = value

    @pl.when(step >= REACH)
    def _():
        upper[0] = value


def rim_copies(moved):
    _, planes, count, cells = moved.shape
    rim = jax.ShapeDtypeStruct((REACH, 2 * count, cells), jnp.bfloat16)
    return pl.pallas_call(
        rim_kernel,
        grid=(2 * REACH,),
        in_specs=[
            pl.BlockSpec(
                (2, 1, count, cells),
                lambda i: (0, jnp.where(i < REACH, i, i + planes - 2 * REACH), 0, 0),
            )
        ],
        out_specs=[
            pl.BlockSpec((1, 2 * count, cells), lambda i: (jnp.minimum(i, REACH - 1), 0, 0)),
            pl.BlockSpec((1, 2 * count, cells), lambda i: (jnp.maximum(i - REACH, 0), 0, 0)),
        ],
        out_shape=[rim, rim],
        name="rim_copies",
    )(moved)


def center_factor(potential, plane, lanes):
    shift = energy_shift + 1.5 * stencil_coeffs[0]
    return (potential[plane : plane + 1, lanes] - shift) * (1.0 / energy_scale)


def across(values, plane, planes):
    total = None
    for offset in range(1, REACH + 1):
        pair = [values(at) for at in (plane - offset, plane + offset) if 0 <= at < planes]
        if pair:
            both = pair[0] + pair[1] if len(pair) == 2 else pair[0]
            term = (0.5 / energy_scale * stencil_coeffs[offset]) * both
            total = term if total is None else total + term
    return total


def first_kernel(current, left, right, potential, table, partial, to_lower, to_upper, copies, values):
    planes = current.shape[1]
    fields = 2 * current.shape[2]
    step = pl.program_id(0)
    last = pl.num_programs(0) - 1
    for plane in range(planes):
        rows = slice(fields * plane, fields * (plane + 1))
        own = joined(current, plane)
        values[rows, :] = own
        copies[rows, MARGIN : MARGIN + CHUNK] = own.astype(jnp.bfloat16)
        before = joined(left, plane)
        after = joined(right, plane)
        copies[rows, :MARGIN] = jnp.where(step == 0, 0.0, before).astype(jnp.bfloat16)
        copies[rows, MARGIN + CHUNK :] = jnp.where(step == last, 0.0, after).astype(jnp.bfloat16)
    for phase in range(CHUNK // TILE):
        lanes = slice(phase * TILE, (phase + 1) * TILE)
        in_plane = jnp.dot(
            copies[:, phase * TILE : phase * TILE + WINDOW], table[phase], preferred_element_type=jnp.float32
        )
        results = []
        for plane in range(planes):
            rows = slice(fields * plane, fields * (plane + 1))
            result = (
                center_factor(potential, plane, lanes) * values[rows, lanes]
                - (0.5 / energy_scale / TABLE_SCALE) * in_plane[rows]
                - across(lambda at: values[fields * at : fields * (at + 1), lanes], plane, planes)
            )
            partial[plane, :, lanes] = result
            results.append(result)
        for rim, into, order in ((to_upper, "up", results[::-1]), (to_lower, "down", results)):
            for plane in range(REACH):
                total = None
                for offset in range(plane + 1, REACH + 1):
                    term = stencil_coeffs[offset] * order[offset - plane - 1]
                    total = term if total is None else total + term
                rim[plane, :, lanes] = total.astype(jnp.bfloat16)


def first_partial(moved, potential, table):
    _, planes, count, cells = moved.shape
    chunks = cells // CHUNK
    margins = CHUNK // MARGIN
    fields = 2 * count
    rim = jax.ShapeDtypeStruct((REACH, fields, cells), jnp.bfloat16)
    rim_spec = pl.BlockSpec((REACH, fields, CHUNK), lambda i: (0, 0, i))
    return pl.pallas_call(
        first_kernel,
        grid=(chunks,),
        in_specs=[
            pl.BlockSpec((2, planes, count, CHUNK), lambda i: (0, 0, 0, i)),
            pl.BlockSpec((2, planes, count, MARGIN), lambda i: (0, 0, 0, jnp.maximum(margins * i - 1, 0))),
            pl.BlockSpec(
                (2, planes, count, MARGIN),
                lambda i: (0, 0, 0, jnp.minimum(margins * (i + 1), margins * chunks - 1)),
            ),
            pl.BlockSpec((planes, CHUNK), lambda i: (0, i)),
            pl.BlockSpec(table.shape, lambda i: (0, 0, 0)),
        ],
        out_specs=[pl.BlockSpec((planes, fields, CHUNK), lambda i: (0, 0, i)), rim_spec, rim_spec],
        out_shape=[jax.ShapeDtypeStruct((planes, fields, cells), jnp.float32), rim, rim],
        scratch_shapes=[
            pltpu.VMEM((planes * fields, CHUNK + 2 * MARGIN), jnp.bfloat16),
            pltpu.VMEM((planes * fields, CHUNK), jnp.float32),
        ],
        cost_estimate=pl.CostEstimate(flops=10**8, transcendentals=0, bytes_accessed=10**7),
        name="first_partial",
    )(moved, moved, moved, potential, table)


def rim_matrix():
    coeffs = stencil_coeffs
    matrix = np.zeros((REACH, REACH))
    for plane in range(REACH):
        for origin in range(REACH):
            for beyond in range(1, REACH + 1):
                if plane + beyond <= REACH and origin + beyond <= REACH:
                    matrix[plane, origin] -= 0.5 / energy_scale * coeffs[plane + beyond] * coeffs[origin + beyond]
    return matrix


def second_kernel(flags, partial, below, above, orbitals, potential, table, out, copies, firsts):
    planes = partial.shape[0]
    fields = partial.shape[1]
    cells = firsts.shape[1]
    step = pl.program_id(0)
    chunks = pl.num_programs(0) - 1
    half_scale = 0.5 / energy_scale

    @pl.when(step == 0)
    def _():
        copies[:, :MARGIN] = jnp.zeros((planes * fields, MARGIN), jnp.bfloat16)
        copies[:, MARGIN + cells :] = jnp.zeros((planes * fields, MARGIN), jnp.bfloat16)

    @pl.when(step < chunks)
    def _():
        base = pl.multiple_of(step * CHUNK, TILE)
        for plane in range(planes):
            rows = slice(fields * plane, fields * (plane + 1))
            first = partial[plane]
            for offset in range(1, REACH + 1):
                if plane - offset < 0:
                    first = first - half_scale * stencil_coeffs[offset] * below[REACH + plane - offset].astype(jnp.float32)
                if plane + offset >= planes:
                    first = first - half_scale * stencil_coeffs[offset] * above[plane + offset - planes].astype(jnp.float32)
            firsts[rows, pl.ds(base, CHUNK)] = first
            copies[rows, pl.ds(pl.multiple_of(base + MARGIN, 128), CHUNK)] = first.astype(jnp.bfloat16)

    @pl.when(step > 0)
    def _():
        base = pl.multiple_of((step - 1) * CHUNK, TILE)
        rim = rim_matrix()
        row = lax.broadcasted_iota(jnp.int32, (fields, TILE), 0)
        turn = jnp.where(row < fields // 2, 2.0 * bessel_terms[1], -2.0 * bessel_terms[1])
        for phase in range(CHUNK // TILE):
            start = pl.multiple_of(base + phase * TILE, TILE)
            lanes = slice(phase * TILE, (phase + 1) * TILE)
            in_plane = jnp.dot(copies[:, pl.ds(start, WINDOW)], table[phase], preferred_element_type=jnp.float32)
            origin = [joined(orbitals, plane, lanes) for plane in range(planes)]
            first = [firsts[fields * plane : fields * (plane + 1), pl.ds(start, TILE)] for plane in range(planes)]
            for plane in range(planes):
                rows = slice(fields * plane, fields * (plane + 1))
                energy = (
                    center_factor(potential, plane, lanes) * first[plane]
                    - (half_scale / TABLE_SCALE) * in_plane[rows]
                    - across(lambda at: first[at], plane, planes)
                )
                result = (
                    (bessel_terms[0] + 2.0 * bessel_terms[2]) * origin[plane]
                    + turn * pltpu.roll(first[plane], fields // 2, 0)
                    - (4.0 * bessel_terms[2]) * energy
                )
                gain = 4.0 * bessel_terms[2] * half_scale
                if plane < REACH:
                    total = sum(float(gain * rim[plane, at]) * origin[at] for at in range(REACH))
                    result = result + flags[0] * total
                mirrored = planes - 1 - plane
                if mirrored < REACH:
                    total = sum(float(gain * rim[mirrored, at]) * origin[planes - 1 - at] for at in range(REACH))
                    result = result + flags[1] * total
                out[plane, :, lanes] = result


def second_partial(flags, partial, below, above, moved, potential, table):
    _, planes, count, cells = moved.shape
    chunks = cells // CHUNK
    fields = 2 * count
    ahead = lambda i: jnp.minimum(i, chunks - 1)
    behind = lambda i: jnp.maximum(i - 1, 0)
    rim_spec = pl.BlockSpec((REACH, fields, CHUNK), lambda i: (0, 0, ahead(i)))
    return pl.pallas_call(
        second_kernel,
        grid=(chunks + 1,),
        in_specs=[
            pl.BlockSpec(memory_space=pltpu.SMEM),
            pl.BlockSpec((planes, fields, CHUNK), lambda i: (0, 0, ahead(i))),
            rim_spec,
            rim_spec,
            pl.BlockSpec((2, planes, count, CHUNK), lambda i: (0, 0, 0, behind(i))),
            pl.BlockSpec((planes, CHUNK), lambda i: (0, behind(i))),
            pl.BlockSpec(table.shape, lambda i: (0, 0, 0)),
        ],
        out_specs=pl.BlockSpec((planes, fields, CHUNK), lambda i: (0, 0, behind(i))),
        out_shape=jax.ShapeDtypeStruct((planes, fields, cells), jnp.float32),
        scratch_shapes=[
            pltpu.VMEM((planes * fields, cells + 2 * MARGIN), jnp.bfloat16),
            pltpu.VMEM((planes * fields, cells), jnp.float32),
        ],
        cost_estimate=pl.CostEstimate(flops=10**8, transcendentals=0, bytes_accessed=10**7),
        name="second_partial",
    )(flags, partial, below, above, moved, potential, table)


def finish_kernel(partial, below, above, weights, out, density):
    planes = partial.shape[0]
    count = out.shape[2]
    gain = 4.0 * bessel_terms[2] * 0.5 / energy_scale
    weight = weights[:, :1]
    for plane in range(planes):
        value = partial[plane]
        if plane < REACH:
            value = value + gain * below[plane].astype(jnp.float32)
        if planes - 1 - plane < REACH:
            value = value + gain * above[planes - 1 - plane].astype(jnp.float32)
        out[0, plane] = value[:count]
        out[1, plane] = value[count:]
        density[plane : plane + 1, :] = jnp.sum(weight * (value * value), axis=0, keepdims=True)


def finish(partial, below, above, weights):
    planes, fields, cells = partial.shape
    chunks = cells // CHUNK
    rim_spec = pl.BlockSpec((REACH, fields, CHUNK), lambda i: (0, 0, i))
    return pl.pallas_call(
        finish_kernel,
        grid=(chunks,),
        in_specs=[
            pl.BlockSpec((planes, fields, CHUNK), lambda i: (0, 0, i)),
            rim_spec,
            rim_spec,
            pl.BlockSpec((fields, 128), lambda i: (0, 0)),
        ],
        out_specs=[
            pl.BlockSpec((2, planes, fields // 2, CHUNK), lambda i: (0, 0, 0, i)),
            pl.BlockSpec((planes, CHUNK), lambda i: (0, i)),
        ],
        out_shape=[
            jax.ShapeDtypeStruct((2, planes, fields // 2, cells), jnp.float32),
            jax.ShapeDtypeStruct((planes, cells), jnp.float32),
        ],
        name="finish",
    )(partial, below, above, weights)


def wave_basis(length):
    cells = np.arange(length)
    rows = []
    waves = []
    for wave in range(length // 2 + 1):
        norm = math.sqrt((1.0 if wave in (0, length / 2) else 2.0) / length)
        rows.append(norm * np.cos(2.0 * math.pi / length * (wave * cells % length)))
        waves.append(wave)
    for wave in range(1, (length + 1) // 2):
        rows.append(math.sqrt(2.0 / length) * np.sin(2.0 * math.pi / length * (wave * cells % length)))
        waves.append(wave)
    return np.asarray(rows, np.float32), (2.0 * math.pi / length * np.asarray(waves, np.float64)) ** 2


def hartree_waves(partial_density):
    planes = partial_density.shape[0]
    bands = lax.axis_size("band")
    blocks = lax.axis_size("space")
    whole = ("band", "space")
    exact = dict(precision=lax.Precision.HIGHEST, preferred_element_type=jnp.float32)
    z_basis, z_squares = wave_basis(NZ)
    y_basis, y_squares = wave_basis(NY)
    x_basis, x_squares = wave_basis(planes * blocks)
    grid = partial_density.reshape(planes, NY, NZ)
    spectral = jnp.einsum("xyz,cz->xyc", grid, z_basis, **exact)
    spectral = jnp.einsum("by,xyc->xbc", y_basis, spectral, **exact)
    columns = lax.all_to_all(spectral, whole, split_axis=1, concat_axis=0, tiled=True)
    rows = columns.shape[1]
    columns = jnp.sum(columns.reshape(bands, planes * blocks, rows, NZ), axis=0)
    place = (lax.axis_index("band") * blocks + lax.axis_index("space")) * rows
    squares = (
        jnp.asarray(x_squares, jnp.float32)[:, None, None]
        + lax.dynamic_slice_in_dim(jnp.asarray(y_squares, jnp.float32), place, rows)[None, :, None]
        + jnp.asarray(z_squares, jnp.float32)[None, None, :]
    )
    kernel = jnp.where(squares > 0, 4.0 * math.pi / jnp.where(squares > 0, squares, 1.0), 0.0)
    columns = jnp.einsum("ax,xbc->abc", x_basis, columns, **exact) * kernel
    columns = jnp.einsum("ax,abc->xbc", x_basis, columns, **exact)
    spread = jnp.broadcast_to(columns[None], (bands, *columns.shape)).reshape(-1, rows, NZ)
    spectral = lax.all_to_all(spread, whole, split_axis=0, concat_axis=1, tiled=True)
    spectral = jnp.einsum("by,xbc->xyc", y_basis, spectral, **exact)
    field = jnp.einsum("cz,xyc->xyz", z_basis, spectral, **exact)
    return field.reshape(planes, NY * NZ)


def ring_shift(x, axis, by):
    count = lax.axis_size(axis)
    return lax.ppermute(x, axis, [(i, (i + by) % count) for i in range(count)])


def band_sum(partial):
    bands = lax.axis_size("band")
    mine = lax.axis_index("band")
    width = partial.shape[1] // bands
    piece = lambda shift: lax.dynamic_slice_in_dim(partial, (mine + shift) % bands * width, width, 1)
    own = piece(0)
    for shift in range(1, bands):
        own = own + ring_shift(piece(shift), "band", shift)
    total = jnp.zeros_like(partial)
    total = lax.dynamic_update_slice_in_dim(total, own, mine * width, 1)
    for shift in range(1, bands):
        arrived = ring_shift(own, "band", shift)
        total = lax.dynamic_update_slice_in_dim(total, arrived, (mine - shift) % bands * width, 1)
    return total


def per_device_blocks(orbitals, potential, occupations):
    count = orbitals.shape[1]
    moved = orbitals.transpose(0, 2, 1, 3)
    table = plane_table()
    place = lax.axis_index("space")
    flags = jnp.stack([place > 0, place < lax.axis_size("space") - 1]).astype(jnp.float32)
    lower, upper = rim_copies(moved)
    below = from_behind(upper, "space", 1)
    above = from_behind(lower, "space", -1)
    partial, to_lower, to_upper = first_partial(moved, potential, table)
    terms_below = from_behind(to_upper, "space", 1)
    terms_above = from_behind(to_lower, "space", -1)
    partial = second_partial(flags, partial, below, above, moved, potential, table)
    weights = occupations / (count * lax.axis_size("band"))
    weights = jnp.broadcast_to(jnp.concatenate([weights, weights])[:, None], (2 * count, 128))
    propagated, partial_density = finish(partial, terms_below, terms_above, weights)
    hartree = hartree_waves(partial_density)
    density = band_sum(partial_density)
    return (propagated.transpose(0, 2, 1, 3), density, hartree)


def per_device(orbitals, potential, occupations):
    _, count, planes, cells = orbitals.shape
    columns = NY % (lax.axis_size("space") * lax.axis_size("band"))
    if planes < 2 * REACH or count != 4 or cells % CHUNK or CHUNK % NZ or MARGIN != REACH * NZ or columns:
        return per_device_general(orbitals, potential, occupations)
    return per_device_blocks(orbitals, potential, occupations)


def solution(mesh):
    in_specs = (P(None, "band", "space", None), P("space", None), P("band"))
    out_specs = (P(None, "band", "space", None), P("space", None), P("space", None))
    return jax.shard_map(
        per_device, mesh=mesh, in_specs=in_specs, out_specs=out_specs, check_vma=False
    )
```

```python
import math

import jax
import jax.numpy as jnp
import numpy as np
from jax import lax
from jax.experimental import pallas as pl
from jax.experimental.pallas import tpu as pltpu
from jax.sharding import PartitionSpec as P

NX = 96
NY = 96
NZ = 96


stencil_coeffs = (-205.0 / 72.0, 8.0 / 5.0, -1.0 / 5.0, 8.0 / 315.0, -1.0 / 560.0)
energy_shift = 6.0
energy_scale = 8.0
bessel_terms = (0.7651976865579666, 0.44005058574493355, 0.11490348493190049)


def from_behind(x, axis, by):
    count = lax.axis_size(axis)
    pairs = [(i, i + by) for i in range(count) if 0 <= i + by < count]
    return lax.ppermute(x, axis, pairs)


def plane_laplace(center, wider):
    reach_cells = len(stencil_coeffs) - 1
    planes = center.shape[-2]
    cells = center.shape[-1]
    spread = wider.astype(jnp.float32)
    middle = spread[..., reach_cells : reach_cells + planes, :]
    summed = 3.0 * stencil_coeffs[0] * center
    for offset in range(1, reach_cells + 1):
        after = spread[..., reach_cells + offset : reach_cells + offset + planes, :]
        before = spread[..., reach_cells - offset : reach_cells - offset + planes, :]
        summed = summed + stencil_coeffs[offset] * (after + before)
    margin = reach_cells * NZ
    padded = jnp.pad(middle, [(0, 0)] * (middle.ndim - 1) + [(margin, margin)])
    z_index = lax.iota(jnp.int32, cells) % NZ
    for offset in range(1, reach_cells + 1):
        stride = offset * NZ
        beyond = padded[..., margin + stride : margin + stride + cells]
        behind = padded[..., margin - stride : margin - stride + cells]
        summed = summed + stencil_coeffs[offset] * (beyond + behind)
        beyond = jnp.where(
            z_index + offset < NZ, padded[..., margin + offset : margin + offset + cells], 0.0
        )
        behind = jnp.where(
            z_index - offset >= 0, padded[..., margin - offset : margin - offset + cells], 0.0
        )
        summed = summed + stencil_coeffs[offset] * (beyond + behind)
    return summed


def scaled_hamiltonian(center, wider, field_values):
    energy = -0.5 * plane_laplace(center, wider) + field_values * center
    return (energy - energy_shift * center) / energy_scale


def slab_rims(source, extent):
    planes = source.shape[-2]
    lower_parts = []
    upper_parts = []
    for distance in range(1, -(-extent // planes) + 1):
        needed = min(planes, extent - (distance - 1) * planes)
        for heading in (1, -1):
            if heading == 1:
                outgoing = source[..., planes - needed :, :]
            else:
                outgoing = source[..., :needed, :]
            arrived = from_behind(outgoing, "space", heading * distance)
            if heading == 1:
                lower_parts.append(arrived)
            else:
                upper_parts.append(arrived)
    return jnp.concatenate(lower_parts[::-1] + [source] + upper_parts, axis=-2)


def dft_tables(length):
    indices = lax.iota(jnp.int32, length)
    product = indices[:, None] * indices[None, :] % length
    phases = 2.0 * math.pi / length * product.astype(jnp.float32)
    return (jnp.cos(phases), jnp.sin(phases))


def turn_axis(cosine, sines, values, pattern):
    direct = jnp.einsum(pattern, cosine, values, precision=lax.Precision.HIGHEST)
    crossed = jnp.einsum(pattern, sines, values, precision=lax.Precision.HIGHEST)
    real_part = direct[..., :NZ] - crossed[..., NZ:]
    imag_part = direct[..., NZ:] + crossed[..., :NZ]
    return jnp.concatenate([real_part, imag_part], axis=-1)


def squared_waves(length, anchor, extent):
    indices = anchor + lax.iota(jnp.int32, extent)
    signed = jnp.where(indices < (length + 1) // 2, indices, indices - length).astype(jnp.float32)
    return (2.0 * math.pi / length * signed) ** 2


def hartree_field(density):
    planes = density.shape[0]
    z_cosine, z_sine = dft_tables(NZ)
    y_cosine, y_sine = dft_tables(NY)
    x_cosine, x_sine = dft_tables(NX)
    forward_z = jnp.concatenate([z_cosine, -z_sine], axis=1)
    flattened = density.reshape(planes * NY, NZ)
    spectral = jnp.dot(
        flattened, forward_z, precision=lax.Precision.HIGHEST, preferred_element_type=jnp.float32
    )
    spectral = turn_axis(y_cosine, -y_sine, spectral.reshape(planes, NY, 2 * NZ), "ky,xyz->xkz")
    columns = lax.all_to_all(spectral, "space", split_axis=1, concat_axis=0, tiled=True)
    y_rows = columns.shape[1]
    spectral = turn_axis(x_cosine, -x_sine, columns, "kx,xyz->kyz")
    squares = (
        squared_waves(NX, 0, NX)[:, None, None]
        + squared_waves(NY, lax.axis_index("space") * y_rows, y_rows)[None, :, None]
        + squared_waves(NZ, 0, NZ)[None, None, :]
    )
    kernel = jnp.where(squares > 0, 4.0 * math.pi / jnp.where(squares > 0, squares, 1.0), 0.0)
    spectral = spectral * jnp.concatenate([kernel, kernel], axis=-1)
    spectral = turn_axis(x_cosine, x_sine, spectral, "kx,xyz->kyz")
    slabs = lax.all_to_all(spectral, "space", split_axis=0, concat_axis=1, tiled=True)
    spectral = turn_axis(y_cosine, y_sine, slabs, "ky,xyz->xkz")
    inverse_z = jnp.concatenate([z_cosine, -z_sine], axis=0)
    field_values = jnp.dot(
        spectral.reshape(planes * NY, 2 * NZ),
        inverse_z,
        precision=lax.Precision.HIGHEST,
        preferred_element_type=jnp.float32,
    )
    return (field_values / (NX * NY * NZ)).reshape(planes, NY * NZ)


def per_device_general(orbitals, potential, occupations):
    reach_cells = len(stencil_coeffs) - 1
    orbital_count = orbitals.shape[1]
    zero_copy = slab_rims(orbitals.astype(jnp.bfloat16), reach_cells)
    first_term = scaled_hamiltonian(orbitals, zero_copy, potential)
    first_copy = slab_rims(first_term.astype(jnp.bfloat16), reach_cells)
    second_term = 2.0 * scaled_hamiltonian(first_term, first_copy, potential) - orbitals
    prop_real = (
        bessel_terms[0] * orbitals[0]
        + 2.0 * bessel_terms[1] * first_term[1]
        - 2.0 * bessel_terms[2] * second_term[0]
    )
    prop_imag = (
        bessel_terms[0] * orbitals[1]
        - 2.0 * bessel_terms[1] * first_term[0]
        - 2.0 * bessel_terms[2] * second_term[1]
    )
    propagated = jnp.stack([prop_real, prop_imag])
    weights = occupations / (orbital_count * lax.axis_size("band"))
    partial_density = jnp.sum(
        weights[:, None, None] * (prop_real * prop_real + prop_imag * prop_imag), axis=0
    )
    density = lax.psum(partial_density, "band")
    hartree = hartree_field(density)
    return (propagated, density, hartree)


REACH = len(stencil_coeffs) - 1
TABLE_SCALE = 5040.0
PERIOD = 768
CHUNK = 2304
WINDOW = 1024
TILE = 256
MARGIN = 384


def plane_table():
    phases = PERIOD // TILE
    table = np.zeros((phases, WINDOW, TILE), np.float32)
    scaled = [round(coeff * TABLE_SCALE) for coeff in stencil_coeffs[1:]]
    for phase in range(phases):
        target = phase * TILE + np.arange(TILE)[None, :]
        origin = phase * TILE - MARGIN + np.arange(WINDOW)[:, None]
        y_step = origin // NZ - target // NZ
        z_step = origin % NZ - target % NZ
        for offset in range(1, REACH + 1):
            along_y = (np.abs(y_step) == offset) & (z_step == 0)
            along_z = (y_step == 0) & (np.abs(z_step) == offset)
            table[phase] += scaled[offset - 1] * (along_y | along_z)
    return jnp.asarray(table, jnp.bfloat16)


def joined(block, plane, lanes=slice(None)):
    return jnp.concatenate([block[0, plane, :, lanes], block[1, plane, :, lanes]], axis=0)


def rim_kernel(orbitals, lower, upper, staged, arrivals):
    planes = orbitals.shape[1]
    starts = (0, planes - REACH)
    copies = [
        pltpu.make_async_copy(orbitals.at[:, pl.ds(start, REACH)], staged.at[side], arrivals.at[side])
        for side, start in enumerate(starts)
    ]
    for copy in copies:
        copy.start()
    for side, rim in enumerate((lower, upper)):
        copies[side].wait()
        for plane in range(REACH):
            rim[plane] = jnp.concatenate([staged[side, 0, plane], staged[side, 1, plane]], axis=0).astype(jnp.bfloat16)


def rim_copies(moved):
    _, planes, count, cells = moved.shape
    rim = jax.ShapeDtypeStruct((REACH, 2 * count, cells), jnp.bfloat16)
    return pl.pallas_call(
        rim_kernel,
        in_specs=[pl.BlockSpec(memory_space=pl.ANY)],
        out_specs=[pl.BlockSpec(memory_space=pltpu.VMEM)] * 2,
        out_shape=[rim, rim],
        scratch_shapes=[
            pltpu.VMEM((2, 2, REACH, count, cells), jnp.float32),
            pltpu.SemaphoreType.DMA((2,)),
        ],
        name="rim_copies",
    )(moved)


def center_factor(potential, plane, lanes):
    shift = energy_shift + 1.5 * stencil_coeffs[0]
    return (potential[plane : plane + 1, lanes] - shift) * (1.0 / energy_scale)


def across(values, plane, planes):
    total = None
    for offset in range(1, REACH + 1):
        pair = [values(at) for at in (plane - offset, plane + offset) if 0 <= at < planes]
        if pair:
            both = pair[0] + pair[1] if len(pair) == 2 else pair[0]
            term = (0.5 / energy_scale * stencil_coeffs[offset]) * both
            total = term if total is None else total + term
    return total


def first_kernel(current, left, right, potential, table, partial, to_lower, to_upper, copies, values):
    planes = current.shape[1]
    fields = 2 * current.shape[2]
    step = pl.program_id(0)
    last = pl.num_programs(0) - 1
    for plane in range(planes):
        rows = slice(fields * plane, fields * (plane + 1))
        own = joined(current, plane)
        values[rows, :] = own
        copies[rows, MARGIN : MARGIN + CHUNK] = own.astype(jnp.bfloat16)
        before = joined(left, plane)
        after = joined(right, plane)
        copies[rows, :MARGIN] = jnp.where(step == 0, 0.0, before).astype(jnp.bfloat16)
        copies[rows, MARGIN + CHUNK :] = jnp.where(step == last, 0.0, after).astype(jnp.bfloat16)
    for phase in range(CHUNK // TILE):
        lanes = slice(phase * TILE, (phase + 1) * TILE)
        in_plane = jnp.dot(
            copies[:, phase * TILE : phase * TILE + WINDOW], table[phase % (PERIOD // TILE)], preferred_element_type=jnp.float32
        )
        results = []
        for plane in range(planes):
            rows = slice(fields * plane, fields * (plane + 1))
            result = (
                center_factor(potential, plane, lanes) * values[rows, lanes]
                - (0.5 / energy_scale / TABLE_SCALE) * in_plane[rows]
                - across(lambda at: values[fields * at : fields * (at + 1), lanes], plane, planes)
            )
            partial[plane, :, lanes] = result
            results.append(result)
        for rim, into, order in ((to_upper, "up", results[::-1]), (to_lower, "down", results)):
            for plane in range(REACH):
                total = None
                for offset in range(plane + 1, REACH + 1):
                    term = stencil_coeffs[offset] * order[offset - plane - 1]
                    total = term if total is None else total + term
                rim[plane, :, lanes] = total.astype(jnp.bfloat16)


def first_partial(moved, potential, table):
    _, planes, count, cells = moved.shape
    chunks = cells // CHUNK
    margins = CHUNK // MARGIN
    fields = 2 * count
    rim = jax.ShapeDtypeStruct((REACH, fields, cells), jnp.bfloat16)
    rim_spec = pl.BlockSpec((REACH, fields, CHUNK), lambda i: (0, 0, i))
    return pl.pallas_call(
        first_kernel,
        grid=(chunks,),
        in_specs=[
            pl.BlockSpec((2, planes, count, CHUNK), lambda i: (0, 0, 0, i)),
            pl.BlockSpec((2, planes, count, MARGIN), lambda i: (0, 0, 0, jnp.maximum(margins * i - 1, 0))),
            pl.BlockSpec(
                (2, planes, count, MARGIN),
                lambda i: (0, 0, 0, jnp.minimum(margins * (i + 1), margins * chunks - 1)),
            ),
            pl.BlockSpec((planes, CHUNK), lambda i: (0, i)),
            pl.BlockSpec(table.shape, lambda i: (0, 0, 0)),
        ],
        out_specs=[pl.BlockSpec((planes, fields, CHUNK), lambda i: (0, 0, i)), rim_spec, rim_spec],
        out_shape=[jax.ShapeDtypeStruct((planes, fields, cells), jnp.float32), rim, rim],
        scratch_shapes=[
            pltpu.VMEM((planes * fields, CHUNK + 2 * MARGIN), jnp.bfloat16),
            pltpu.VMEM((planes * fields, CHUNK), jnp.float32),
        ],
        cost_estimate=pl.CostEstimate(flops=10**8, transcendentals=0, bytes_accessed=10**7),
        name="first_partial",
    )(moved, moved, moved, potential, table)


def rim_matrix():
    coeffs = stencil_coeffs
    matrix = np.zeros((REACH, REACH))
    for plane in range(REACH):
        for origin in range(REACH):
            for beyond in range(1, REACH + 1):
                if plane + beyond <= REACH and origin + beyond <= REACH:
                    matrix[plane, origin] -= 0.5 / energy_scale * coeffs[plane + beyond] * coeffs[origin + beyond]
    return matrix


def second_kernel(partial, below, above, orbitals, potential, table, out, copies, firsts):
    planes = partial.shape[0]
    fields = partial.shape[1]
    cells = firsts.shape[1]
    step = pl.program_id(0)
    chunks = pl.num_programs(0) - 1
    half_scale = 0.5 / energy_scale
    place = lax.axis_index("space")
    flags = [(place > 0).astype(jnp.float32), (place < lax.axis_size("space") - 1).astype(jnp.float32)]

    @pl.when(step == 0)
    def _():
        copies[:, :MARGIN] = jnp.zeros((planes * fields, MARGIN), jnp.bfloat16)
        copies[:, MARGIN + cells :] = jnp.zeros((planes * fields, MARGIN), jnp.bfloat16)

    @pl.when(step < chunks)
    def _():
        base = pl.multiple_of(step * CHUNK, TILE)
        for plane in range(planes):
            rows = slice(fields * plane, fields * (plane + 1))
            first = partial[plane]
            for offset in range(1, REACH + 1):
                if plane - offset < 0:
                    first = first - half_scale * stencil_coeffs[offset] * below[REACH + plane - offset].astype(jnp.float32)
                if plane + offset >= planes:
                    first = first - half_scale * stencil_coeffs[offset] * above[plane + offset - planes].astype(jnp.float32)
            firsts[rows, pl.ds(base, CHUNK)] = first
            copies[rows, pl.ds(pl.multiple_of(base + MARGIN, 128), CHUNK)] = first.astype(jnp.bfloat16)

    @pl.when(step > 0)
    def _():
        base = pl.multiple_of((step - 1) * CHUNK, TILE)
        rim = rim_matrix()
        row = lax.broadcasted_iota(jnp.int32, (fields, TILE), 0)
        turn = jnp.where(row < fields // 2, 2.0 * bessel_terms[1], -2.0 * bessel_terms[1])
        for phase in range(CHUNK // TILE):
            start = pl.multiple_of(base + phase * TILE, TILE)
            lanes = slice(phase * TILE, (phase + 1) * TILE)
            in_plane = jnp.dot(copies[:, pl.ds(start, WINDOW)], table[phase % (PERIOD // TILE)], preferred_element_type=jnp.float32)
            origin = [joined(orbitals, plane, lanes) for plane in range(planes)]
            first = [firsts[fields * plane : fields * (plane + 1), pl.ds(start, TILE)] for plane in range(planes)]
            for plane in range(planes):
                rows = slice(fields * plane, fields * (plane + 1))
                energy = (
                    center_factor(potential, plane, lanes) * first[plane]
                    - (half_scale / TABLE_SCALE) * in_plane[rows]
                    - across(lambda at: first[at], plane, planes)
                )
                result = (
                    (bessel_terms[0] + 2.0 * bessel_terms[2]) * origin[plane]
                    + turn * pltpu.roll(first[plane], fields // 2, 0)
                    - (4.0 * bessel_terms[2]) * energy
                )
                gain = 4.0 * bessel_terms[2] * half_scale
                if plane < REACH:
                    total = sum(float(gain * rim[plane, at]) * origin[at] for at in range(REACH))
                    result = result + flags[0] * total
                mirrored = planes - 1 - plane
                if mirrored < REACH:
                    total = sum(float(gain * rim[mirrored, at]) * origin[planes - 1 - at] for at in range(REACH))
                    result = result + flags[1] * total
                out[plane, :, lanes] = result


def second_partial(partial, below, above, moved, potential, table):
    _, planes, count, cells = moved.shape
    chunks = cells // CHUNK
    fields = 2 * count
    ahead = lambda i: jnp.minimum(i, chunks - 1)
    behind = lambda i: jnp.maximum(i - 1, 0)
    rim_spec = pl.BlockSpec((REACH, fields, CHUNK), lambda i: (0, 0, ahead(i)))
    return pl.pallas_call(
        second_kernel,
        grid=(chunks + 1,),
        in_specs=[
            pl.BlockSpec((planes, fields, CHUNK), lambda i: (0, 0, ahead(i))),
            rim_spec,
            rim_spec,
            pl.BlockSpec((2, planes, count, CHUNK), lambda i: (0, 0, 0, behind(i))),
            pl.BlockSpec((planes, CHUNK), lambda i: (0, behind(i))),
            pl.BlockSpec(table.shape, lambda i: (0, 0, 0)),
        ],
        out_specs=pl.BlockSpec((planes, fields, CHUNK), lambda i: (0, 0, behind(i))),
        out_shape=jax.ShapeDtypeStruct((planes, fields, cells), jnp.float32),
        scratch_shapes=[
            pltpu.VMEM((planes * fields, cells + 2 * MARGIN), jnp.bfloat16),
            pltpu.VMEM((planes * fields, cells), jnp.float32),
        ],
        cost_estimate=pl.CostEstimate(flops=10**8, transcendentals=0, bytes_accessed=10**7),
        name="second_partial",
    )(partial, below, above, moved, potential, table)


BLOCK = 384
LANES = 128
EXACT = dict(precision=lax.Precision.HIGHEST, preferred_element_type=jnp.float32)


def power_over(peak):
    lift = 14.0 - jnp.floor(jnp.log2(jnp.where(peak > 0.0, peak, 1.0)))
    return jnp.clip(lift, -110.0, 110.0)


def packed(values, lift):
    scaled = values * jnp.exp2(lift)
    lane = lax.broadcasted_iota(jnp.int32, scaled.shape, 1)
    coarse = scaled.astype(jnp.bfloat16).astype(jnp.float32)
    rest = (scaled - coarse)[:, :1]
    scaled = jnp.where(lane == 0, coarse, scaled)
    scaled = jnp.where(lane == NZ, lift, scaled)
    return jnp.where(lane == NZ + 1, rest, scaled)


def unpacked(block):
    lane = lax.broadcasted_iota(jnp.int32, block.shape, 1)
    whole = jnp.where(lane == 0, block + block[:, NZ + 1 : NZ + 2], block)
    return jnp.where(lane < NZ, whole * jnp.exp2(-block[:, NZ : NZ + 1]), 0.0)


def spread_table(block, table):
    table[...] = jnp.zeros(table.shape, table.dtype)
    for part in range(BLOCK // NZ):
        table[part * NZ : (part + 1) * NZ, part * LANES : (part + 1) * LANES] = block[...]


def finish_kernel(shares, partial, below, above, z_block, y_table, out, chunks, z_table, rows, along_z, along_y, sent):
    planes = partial.shape[0]
    fields = partial.shape[1]
    count = fields // 2
    groups = rows.shape[0]
    members = chunks.shape[0]
    step = pl.program_id(0)
    per_step = CHUNK // BLOCK
    gain = 4.0 * bessel_terms[2] * 0.5 / energy_scale
    field = lax.broadcasted_iota(jnp.int32, (fields, 1), 0) % count
    weight = jnp.zeros((fields, 1), jnp.float32)
    for at in range(count):
        weight = jnp.where(field == at, shares[at], weight)
    weight = weight * (1.0 / (count * lax.axis_size("band")))
    for plane in range(planes):
        value = partial[plane]
        if plane < REACH:
            value = value + gain * below[plane].astype(jnp.float32)
        if planes - 1 - plane < REACH:
            value = value + gain * above[planes - 1 - plane].astype(jnp.float32)
        out[0, plane] = value[:count]
        out[1, plane] = value[count:]
        total = jnp.sum(weight * (value * value), axis=0, keepdims=True)
        for group in range(per_step):
            rows[step * per_step + group, plane : plane + 1, :] = total[:, group * BLOCK : (group + 1) * BLOCK]

    @pl.when(step == pl.num_programs(0) - 1)
    def _():
        padded = rows.shape[1]
        spread_table(z_block, z_table)
        turned = jnp.dot(rows[...].reshape(groups * padded, BLOCK), z_table[...], **EXACT)
        for part in range(BLOCK // NZ):
            along_z[part] = turned[:, part * LANES : (part + 1) * LANES]
        for plane in range(planes):
            for part in range(BLOCK // NZ):
                along_y[part * groups : (part + 1) * groups, plane * LANES : (plane + 1) * LANES] = along_z[
                    part, pl.ds(plane, groups, stride=padded), :
                ]
        waves = jnp.dot(y_table[...], along_y[...], **EXACT)
        peak = jnp.max(jnp.max(jnp.abs(waves), axis=1, keepdims=True), axis=0, keepdims=True)
        lift = power_over(peak)
        for part in range(chunks.shape[3] // LANES):
            for plane in range(planes):
                block = waves[part * members : (part + 1) * members, plane * LANES : (plane + 1) * LANES]
                sent[part, pl.ds(plane, members, stride=planes), :] = packed(block, lift)
        for member in range(members):
            for quarter in range(planes // 4):
                start = member * planes + quarter * 4
                for part in range(chunks.shape[3] // LANES):
                    lanes = slice(part * LANES, (part + 1) * LANES)
                    chunks[member, quarter, :, lanes] = sent[part, start : start + 4, :]


def finish(partial, below, above, occupations, z_table, y_table, members):
    planes, fields, cells = partial.shape
    rim_spec = pl.BlockSpec((REACH, fields, CHUNK), lambda i: (0, 0, i))
    groups = cells // BLOCK
    padded = -(-planes // 8) * 8
    width = NY // members * LANES
    whole = lambda shape: pl.BlockSpec(shape, lambda i: (0,) * len(shape))
    wave_shape = (members, planes // 4, 4, width)
    return pl.pallas_call(
        finish_kernel,
        grid=(cells // CHUNK,),
        in_specs=[
            pl.BlockSpec(memory_space=pltpu.SMEM),
            pl.BlockSpec((planes, fields, CHUNK), lambda i: (0, 0, i)),
            rim_spec,
            rim_spec,
            whole(z_table.shape),
            whole(y_table.shape),
        ],
        out_specs=[pl.BlockSpec((2, planes, fields // 2, CHUNK), lambda i: (0, 0, 0, i)), whole(wave_shape)],
        out_shape=[
            jax.ShapeDtypeStruct((2, planes, fields // 2, cells), jnp.float32),
            jax.ShapeDtypeStruct(wave_shape, jnp.float32),
        ],
        scratch_shapes=[
            pltpu.VMEM((BLOCK, BLOCK // NZ * LANES), jnp.float32),
            pltpu.VMEM((groups, padded, BLOCK), jnp.float32),
            pltpu.VMEM((BLOCK // NZ, groups * padded, LANES), jnp.float32),
            pltpu.VMEM((NY, planes * LANES), jnp.float32),
            pltpu.VMEM((width // LANES, members * planes, LANES), jnp.float32),
        ],
        name="finish",
    )(occupations, partial, below, above, z_table, y_table)


def column_kernel(arrived, multiplier, x_table, back_table, chunks, raw, columns, both):
    members, quarters, _, width = arrived.shape
    planes = quarters * 4
    blocks = chunks.shape[0]
    length = blocks * planes
    for member in range(members):
        for quarter in range(quarters):
            start = member * planes + quarter * 4
            raw[start : start + 4, :] = arrived[member, quarter]
    for part in range(width // LANES):
        lanes = slice(part * LANES, (part + 1) * LANES)
        total = unpacked(raw[:length, lanes])
        for band in range(1, members // blocks):
            total = total + unpacked(raw[band * length : (band + 1) * length, lanes])
        columns[:, lanes] = total
    waves = jnp.dot(x_table[...], columns[...], **EXACT) * multiplier[...]
    field = jnp.dot(back_table[...], waves, **EXACT)
    for index, values in enumerate((columns[...], field)):
        peak = jnp.max(jnp.max(jnp.abs(values), axis=1, keepdims=True), axis=0, keepdims=True)
        lift = power_over(peak)
        for part in range(width // LANES):
            at = index * width + part * LANES
            both[:, at : at + LANES] = packed(values[:, part * LANES : (part + 1) * LANES], lift)
    for block in range(blocks):
        for quarter in range(quarters):
            start = block * planes + quarter * 4
            chunks[block, quarter] = both[start : start + 4, :]


def column_waves(arrived, multiplier, x_table, blocks):
    members, quarters, _, width = arrived.shape
    length = x_table.shape[0]
    return pl.pallas_call(
        column_kernel,
        out_shape=jax.ShapeDtypeStruct((blocks, quarters, 4, 2 * width), jnp.float32),
        scratch_shapes=[
            pltpu.VMEM((members * quarters * 4, width), jnp.float32),
            pltpu.VMEM((length, width), jnp.float32),
            pltpu.VMEM((length, 2 * width), jnp.float32),
        ],
        name="column_waves",
    )(arrived, multiplier, jnp.asarray(x_table), jnp.asarray(x_table.T))


def return_kernel(arrived, y_back, z_block, density, hartree, z_table, raw, along_y, along_z, result):
    members, quarters, _, width = arrived.shape
    width //= 2
    planes = quarters * 4
    groups = result.shape[1] // planes
    spread_table(z_block, z_table)
    for member in range(members):
        for quarter in range(quarters):
            start = member * planes + quarter * 4
            for part in range(2 * width // LANES):
                raw[part, start : start + 4, :] = arrived[member, quarter, :, part * LANES : (part + 1) * LANES]
    for index, out in enumerate((density, hartree)):
        for plane in range(planes):
            for part in range(width // LANES):
                block = raw[index * (width // LANES) + part, pl.ds(plane, members, stride=planes), :]
                along_y[part * members : (part + 1) * members, plane * LANES : (plane + 1) * LANES] = unpacked(block)
        waves = jnp.dot(y_back[...], along_y[...], **EXACT)
        for plane in range(planes):
            for part in range(BLOCK // NZ):
                along_z[plane * groups : (plane + 1) * groups, part * LANES : (part + 1) * LANES] = waves[
                    part * groups : (part + 1) * groups, plane * LANES : (plane + 1) * LANES
                ]
        cells = lax.dot_general(along_z[...], z_table[...], (((1,), (1,)), ((), ())), **EXACT)
        for tile in range(BLOCK // LANES):
            result[tile] = cells[:, tile * LANES : (tile + 1) * LANES]
        for group in range(groups):
            for tile in range(BLOCK // LANES):
                at = group * BLOCK + tile * LANES
                out[:, at : at + LANES] = result[tile, pl.ds(group, planes, stride=groups), :]


def return_waves(arrived, y_table, z_table, cells):
    members, quarters, _, width = arrived.shape
    planes = quarters * 4
    groups = cells // BLOCK
    plane_shape = jax.ShapeDtypeStruct((planes, cells), jnp.float32)
    return pl.pallas_call(
        return_kernel,
        out_shape=[plane_shape, plane_shape],
        scratch_shapes=[
            pltpu.VMEM((BLOCK, BLOCK // NZ * LANES), jnp.float32),
            pltpu.VMEM((width // LANES, members * planes, LANES), jnp.float32),
            pltpu.VMEM((NY, planes * LANES), jnp.float32),
            pltpu.VMEM((planes * groups, BLOCK // NZ * LANES), jnp.float32),
            pltpu.VMEM((BLOCK // LANES, planes * groups, LANES), jnp.float32),
        ],
        name="return_waves",
    )(arrived, y_table, z_table)


def wave_basis(length):
    cells = np.arange(length)
    rows = []
    waves = []
    for wave in range(length // 2 + 1):
        norm = math.sqrt((1.0 if wave in (0, length / 2) else 2.0) / length)
        rows.append(norm * np.cos(2.0 * math.pi / length * (wave * cells % length)))
        waves.append(wave)
    for wave in range(1, (length + 1) // 2):
        rows.append(math.sqrt(2.0 / length) * np.sin(2.0 * math.pi / length * (wave * cells % length)))
        waves.append(wave)
    return np.asarray(rows, np.float32), (2.0 * math.pi / length * np.asarray(waves, np.float64)) ** 2


def wave_tables(members, length):
    z_basis, z_squares = wave_basis(NZ)
    y_basis, y_squares = wave_basis(NY)
    x_basis, x_squares = wave_basis(length)
    parts = BLOCK // NZ
    z_table = np.pad(z_basis.T, ((0, 0), (0, LANES - NZ)))
    rows = NY // members
    y_table = y_basis.reshape(members, rows, NY // parts, parts).transpose(1, 0, 3, 2).reshape(NY, NY)
    return z_table, y_table, x_basis, (x_squares, y_squares, z_squares)


def density_and_field(waves, tables, cells):
    bands = lax.axis_size("band")
    blocks = lax.axis_size("space")
    members, quarters, _, width = waves.shape
    z_table, y_table, x_table, (x_squares, y_squares, z_squares) = tables
    exchange = lambda chunks: lax.all_to_all(
        chunks.astype(jnp.float16), ("band", "space"), split_axis=0, concat_axis=0, tiled=True
    ).astype(jnp.float32)
    rows = NY // members
    place = (lax.axis_index("band") * blocks + lax.axis_index("space")) * rows
    squares = (
        jnp.asarray(x_squares, jnp.float32)[:, None, None]
        + lax.dynamic_slice_in_dim(jnp.asarray(y_squares, jnp.float32), place, rows)[None, :, None]
        + jnp.asarray(np.pad(z_squares, (0, LANES - NZ)), jnp.float32)[None, None, :]
    )
    used = lax.broadcasted_iota(jnp.int32, squares.shape, 2) < NZ
    multiplier = jnp.where(
        (squares > 0) & used, 4.0 * math.pi / jnp.where(squares > 0, squares, 1.0), 0.0
    ).reshape(-1, width)
    both = column_waves(exchange(waves), multiplier, x_table, blocks)
    spread = jnp.broadcast_to(both.astype(jnp.float16)[None], (bands, *both.shape)).reshape(members, *both.shape[1:])
    return return_waves(exchange(spread), jnp.asarray(y_table.T), jnp.asarray(z_table), cells)


def per_device_blocks(orbitals, potential, occupations):
    moved = orbitals.transpose(0, 2, 1, 3)
    table = plane_table()
    lower, upper = rim_copies(moved)
    below = from_behind(upper, "space", 1)
    above = from_behind(lower, "space", -1)
    partial, to_lower, to_upper = first_partial(moved, potential, table)
    terms_below = from_behind(to_upper, "space", 1)
    terms_above = from_behind(to_lower, "space", -1)
    partial = second_partial(partial, below, above, moved, potential, table)
    members = lax.axis_size("band") * lax.axis_size("space")
    tables = wave_tables(members, orbitals.shape[2] * lax.axis_size("space"))
    propagated, waves = finish(
        partial, terms_below, terms_above, occupations, jnp.asarray(tables[0]), jnp.asarray(tables[1]), members
    )
    density, hartree = density_and_field(waves, tables, orbitals.shape[3])
    return (propagated.transpose(0, 2, 1, 3), density, hartree)


def per_device(orbitals, potential, occupations):
    _, count, planes, cells = orbitals.shape
    columns = NY % (lax.axis_size("space") * lax.axis_size("band"))
    if planes < 2 * REACH or planes % 4 or count != 4 or cells % CHUNK or PERIOD % NZ or MARGIN != REACH * NZ or columns:
        return per_device_general(orbitals, potential, occupations)
    return per_device_blocks(orbitals, potential, occupations)


def solution(mesh):
    in_specs = (P(None, "band", "space", None), P("space", None), P("band"))
    out_specs = (P(None, "band", "space", None), P("space", None), P("space", None))
    return jax.shard_map(
        per_device, mesh=mesh, in_specs=in_specs, out_specs=out_specs, check_vma=False
    )
```

```python
import math

import jax
import jax.numpy as jnp
import numpy as np
from jax import lax
from jax.experimental import pallas as pl
from jax.experimental.pallas import tpu as pltpu
from jax.sharding import PartitionSpec as P

NX = 96
NY = 96
NZ = 96


stencil_coeffs = (-205.0 / 72.0, 8.0 / 5.0, -1.0 / 5.0, 8.0 / 315.0, -1.0 / 560.0)
energy_shift = 6.0
energy_scale = 8.0
bessel_terms = (0.7651976865579666, 0.44005058574493355, 0.11490348493190049)


def from_behind(x, axis, by):
    count = lax.axis_size(axis)
    pairs = [(i, i + by) for i in range(count) if 0 <= i + by < count]
    return lax.ppermute(x, axis, pairs)


def plane_laplace(center, wider):
    reach_cells = len(stencil_coeffs) - 1
    planes = center.shape[-2]
    cells = center.shape[-1]
    spread = wider.astype(jnp.float32)
    middle = spread[..., reach_cells : reach_cells + planes, :]
    summed = 3.0 * stencil_coeffs[0] * center
    for offset in range(1, reach_cells + 1):
        after = spread[..., reach_cells + offset : reach_cells + offset + planes, :]
        before = spread[..., reach_cells - offset : reach_cells - offset + planes, :]
        summed = summed + stencil_coeffs[offset] * (after + before)
    margin = reach_cells * NZ
    padded = jnp.pad(middle, [(0, 0)] * (middle.ndim - 1) + [(margin, margin)])
    z_index = lax.iota(jnp.int32, cells) % NZ
    for offset in range(1, reach_cells + 1):
        stride = offset * NZ
        beyond = padded[..., margin + stride : margin + stride + cells]
        behind = padded[..., margin - stride : margin - stride + cells]
        summed = summed + stencil_coeffs[offset] * (beyond + behind)
        beyond = jnp.where(
            z_index + offset < NZ, padded[..., margin + offset : margin + offset + cells], 0.0
        )
        behind = jnp.where(
            z_index - offset >= 0, padded[..., margin - offset : margin - offset + cells], 0.0
        )
        summed = summed + stencil_coeffs[offset] * (beyond + behind)
    return summed


def scaled_hamiltonian(center, wider, field_values):
    energy = -0.5 * plane_laplace(center, wider) + field_values * center
    return (energy - energy_shift * center) / energy_scale


def slab_rims(source, extent):
    planes = source.shape[-2]
    lower_parts = []
    upper_parts = []
    for distance in range(1, -(-extent // planes) + 1):
        needed = min(planes, extent - (distance - 1) * planes)
        for heading in (1, -1):
            if heading == 1:
                outgoing = source[..., planes - needed :, :]
            else:
                outgoing = source[..., :needed, :]
            arrived = from_behind(outgoing, "space", heading * distance)
            if heading == 1:
                lower_parts.append(arrived)
            else:
                upper_parts.append(arrived)
    return jnp.concatenate(lower_parts[::-1] + [source] + upper_parts, axis=-2)


def dft_tables(length):
    indices = lax.iota(jnp.int32, length)
    product = indices[:, None] * indices[None, :] % length
    phases = 2.0 * math.pi / length * product.astype(jnp.float32)
    return (jnp.cos(phases), jnp.sin(phases))


def turn_axis(cosine, sines, values, pattern):
    direct = jnp.einsum(pattern, cosine, values, precision=lax.Precision.HIGHEST)
    crossed = jnp.einsum(pattern, sines, values, precision=lax.Precision.HIGHEST)
    real_part = direct[..., :NZ] - crossed[..., NZ:]
    imag_part = direct[..., NZ:] + crossed[..., :NZ]
    return jnp.concatenate([real_part, imag_part], axis=-1)


def squared_waves(length, anchor, extent):
    indices = anchor + lax.iota(jnp.int32, extent)
    signed = jnp.where(indices < (length + 1) // 2, indices, indices - length).astype(jnp.float32)
    return (2.0 * math.pi / length * signed) ** 2


def hartree_field(density):
    planes = density.shape[0]
    z_cosine, z_sine = dft_tables(NZ)
    y_cosine, y_sine = dft_tables(NY)
    x_cosine, x_sine = dft_tables(NX)
    forward_z = jnp.concatenate([z_cosine, -z_sine], axis=1)
    flattened = density.reshape(planes * NY, NZ)
    spectral = jnp.dot(
        flattened, forward_z, precision=lax.Precision.HIGHEST, preferred_element_type=jnp.float32
    )
    spectral = turn_axis(y_cosine, -y_sine, spectral.reshape(planes, NY, 2 * NZ), "ky,xyz->xkz")
    columns = lax.all_to_all(spectral, "space", split_axis=1, concat_axis=0, tiled=True)
    y_rows = columns.shape[1]
    spectral = turn_axis(x_cosine, -x_sine, columns, "kx,xyz->kyz")
    squares = (
        squared_waves(NX, 0, NX)[:, None, None]
        + squared_waves(NY, lax.axis_index("space") * y_rows, y_rows)[None, :, None]
        + squared_waves(NZ, 0, NZ)[None, None, :]
    )
    kernel = jnp.where(squares > 0, 4.0 * math.pi / jnp.where(squares > 0, squares, 1.0), 0.0)
    spectral = spectral * jnp.concatenate([kernel, kernel], axis=-1)
    spectral = turn_axis(x_cosine, x_sine, spectral, "kx,xyz->kyz")
    slabs = lax.all_to_all(spectral, "space", split_axis=0, concat_axis=1, tiled=True)
    spectral = turn_axis(y_cosine, y_sine, slabs, "ky,xyz->xkz")
    inverse_z = jnp.concatenate([z_cosine, -z_sine], axis=0)
    field_values = jnp.dot(
        spectral.reshape(planes * NY, 2 * NZ),
        inverse_z,
        precision=lax.Precision.HIGHEST,
        preferred_element_type=jnp.float32,
    )
    return (field_values / (NX * NY * NZ)).reshape(planes, NY * NZ)


def per_device_general(orbitals, potential, occupations):
    reach_cells = len(stencil_coeffs) - 1
    orbital_count = orbitals.shape[1]
    zero_copy = slab_rims(orbitals.astype(jnp.bfloat16), reach_cells)
    first_term = scaled_hamiltonian(orbitals, zero_copy, potential)
    first_copy = slab_rims(first_term.astype(jnp.bfloat16), reach_cells)
    second_term = 2.0 * scaled_hamiltonian(first_term, first_copy, potential) - orbitals
    prop_real = (
        bessel_terms[0] * orbitals[0]
        + 2.0 * bessel_terms[1] * first_term[1]
        - 2.0 * bessel_terms[2] * second_term[0]
    )
    prop_imag = (
        bessel_terms[0] * orbitals[1]
        - 2.0 * bessel_terms[1] * first_term[0]
        - 2.0 * bessel_terms[2] * second_term[1]
    )
    propagated = jnp.stack([prop_real, prop_imag])
    weights = occupations / (orbital_count * lax.axis_size("band"))
    partial_density = jnp.sum(
        weights[:, None, None] * (prop_real * prop_real + prop_imag * prop_imag), axis=0
    )
    density = lax.psum(partial_density, "band")
    hartree = hartree_field(density)
    return (propagated, density, hartree)


REACH = len(stencil_coeffs) - 1
TABLE_SCALE = 5040.0
PERIOD = 768
CHUNK = 2304
WIDE_CHUNK = 4608
WINDOW = 1024
TILE = 256
MARGIN = 384


def plane_table():
    phases = PERIOD // TILE
    table = np.zeros((phases, WINDOW, TILE), np.float32)
    scaled = [round(coeff * TABLE_SCALE) for coeff in stencil_coeffs[1:]]
    for phase in range(phases):
        target = phase * TILE + np.arange(TILE)[None, :]
        origin = phase * TILE - MARGIN + np.arange(WINDOW)[:, None]
        y_step = origin // NZ - target // NZ
        z_step = origin % NZ - target % NZ
        for offset in range(1, REACH + 1):
            along_y = (np.abs(y_step) == offset) & (z_step == 0)
            along_z = (y_step == 0) & (np.abs(z_step) == offset)
            table[phase] += scaled[offset - 1] * (along_y | along_z)
    return jnp.asarray(table, jnp.bfloat16)


def joined(block, plane, lanes=slice(None)):
    return jnp.concatenate([block[0, plane, :, lanes], block[1, plane, :, lanes]], axis=0)


def rim_kernel(orbitals, lower, upper, staged, arrivals):
    planes = orbitals.shape[1]
    starts = (0, planes - REACH)
    copies = [
        pltpu.make_async_copy(orbitals.at[:, pl.ds(start, REACH)], staged.at[side], arrivals.at[side])
        for side, start in enumerate(starts)
    ]
    for copy in copies:
        copy.start()
    for side, rim in enumerate((lower, upper)):
        copies[side].wait()
        for plane in range(REACH):
            rim[plane] = jnp.concatenate([staged[side, 0, plane], staged[side, 1, plane]], axis=0).astype(jnp.bfloat16)


def rim_copies(moved):
    _, planes, count, cells = moved.shape
    rim = pltpu.VMEM((REACH, 2 * count, cells), jnp.bfloat16)
    return pl.pallas_call(
        rim_kernel,
        in_specs=[pl.BlockSpec(memory_space=pl.ANY)],
        out_specs=[pl.BlockSpec(memory_space=pltpu.VMEM)] * 2,
        out_shape=[rim, rim],
        scratch_shapes=[
            pltpu.VMEM((2, 2, REACH, count, cells), jnp.float32),
            pltpu.SemaphoreType.DMA((2,)),
        ],
        name="rim_copies",
    )(moved)


def center_factor(potential, plane, lanes):
    shift = energy_shift + 1.5 * stencil_coeffs[0]
    return (potential[plane : plane + 1, lanes] - shift) * (1.0 / energy_scale)


def across(values, plane, planes):
    total = None
    for offset in range(1, REACH + 1):
        pair = [values(at) for at in (plane - offset, plane + offset) if 0 <= at < planes]
        if pair:
            both = pair[0] + pair[1] if len(pair) == 2 else pair[0]
            term = (0.5 / energy_scale * stencil_coeffs[offset]) * both
            total = term if total is None else total + term
    return total


def first_kernel(current, left, right, potential, table, partial, to_lower, to_upper, copies, values):
    planes = current.shape[1]
    fields = 2 * current.shape[2]
    step = pl.program_id(0)
    last = pl.num_programs(0) - 1
    for plane in range(planes):
        rows = slice(fields * plane, fields * (plane + 1))
        own = joined(current, plane)
        values[rows, :] = own
        copies[rows, MARGIN : MARGIN + CHUNK] = own.astype(jnp.bfloat16)
        before = joined(left, plane)
        after = joined(right, plane)
        copies[rows, :MARGIN] = jnp.where(step == 0, 0.0, before).astype(jnp.bfloat16)
        copies[rows, MARGIN + CHUNK :] = jnp.where(step == last, 0.0, after).astype(jnp.bfloat16)
    for phase in range(CHUNK // TILE):
        lanes = slice(phase * TILE, (phase + 1) * TILE)
        in_plane = jnp.dot(
            copies[:, phase * TILE : phase * TILE + WINDOW], table[phase % (PERIOD // TILE)], preferred_element_type=jnp.float32
        )
        results = []
        for plane in range(planes):
            rows = slice(fields * plane, fields * (plane + 1))
            result = (
                center_factor(potential, plane, lanes) * values[rows, lanes]
                - (0.5 / energy_scale / TABLE_SCALE) * in_plane[rows]
                - across(lambda at: values[fields * at : fields * (at + 1), lanes], plane, planes)
            )
            partial[plane, :, lanes] = result
            results.append(result)
        for rim, into, order in ((to_upper, "up", results[::-1]), (to_lower, "down", results)):
            for plane in range(REACH):
                total = None
                for offset in range(plane + 1, REACH + 1):
                    term = stencil_coeffs[offset] * order[offset - plane - 1]
                    total = term if total is None else total + term
                rim[plane, :, pl.ds(pl.multiple_of(step * CHUNK + phase * TILE, TILE), TILE)] = total.astype(jnp.bfloat16)


def first_partial(moved, potential, table):
    _, planes, count, cells = moved.shape
    chunks = cells // CHUNK
    margins = CHUNK // MARGIN
    fields = 2 * count
    rim = pltpu.VMEM((REACH, fields, cells), jnp.bfloat16)
    rim_spec = pl.BlockSpec(memory_space=pltpu.VMEM)
    return pl.pallas_call(
        first_kernel,
        grid=(chunks,),
        in_specs=[
            pl.BlockSpec((2, planes, count, CHUNK), lambda i: (0, 0, 0, i)),
            pl.BlockSpec((2, planes, count, MARGIN), lambda i: (0, 0, 0, jnp.maximum(margins * i - 1, 0))),
            pl.BlockSpec(
                (2, planes, count, MARGIN),
                lambda i: (0, 0, 0, jnp.minimum(margins * (i + 1), margins * chunks - 1)),
            ),
            pl.BlockSpec((planes, CHUNK), lambda i: (0, i)),
            pl.BlockSpec(table.shape, lambda i: (0, 0, 0)),
        ],
        out_specs=[pl.BlockSpec((planes, fields, CHUNK), lambda i: (0, 0, i)), rim_spec, rim_spec],
        out_shape=[jax.ShapeDtypeStruct((planes, fields, cells), jnp.float32), rim, rim],
        scratch_shapes=[
            pltpu.VMEM((planes * fields, CHUNK + 2 * MARGIN), jnp.bfloat16),
            pltpu.VMEM((planes * fields, CHUNK), jnp.float32),
        ],
        cost_estimate=pl.CostEstimate(flops=10**8, transcendentals=0, bytes_accessed=10**7),
        name="first_partial",
    )(moved, moved, moved, potential, table)


def rim_matrix():
    coeffs = stencil_coeffs
    matrix = np.zeros((REACH, REACH))
    for plane in range(REACH):
        for origin in range(REACH):
            for beyond in range(1, REACH + 1):
                if plane + beyond <= REACH and origin + beyond <= REACH:
                    matrix[plane, origin] -= 0.5 / energy_scale * coeffs[plane + beyond] * coeffs[origin + beyond]
    return matrix


def second_kernel(partial, below, above, orbitals, potential, table, out, copies, firsts):
    planes = partial.shape[0]
    fields = partial.shape[1]
    cells = firsts.shape[1]
    step = pl.program_id(0)
    chunks = pl.num_programs(0) - 1
    half_scale = 0.5 / energy_scale
    place = lax.axis_index("space")
    flags = [(place > 0).astype(jnp.float32), (place < lax.axis_size("space") - 1).astype(jnp.float32)]

    @pl.when(step == 0)
    def _():
        copies[:, :MARGIN] = jnp.zeros((planes * fields, MARGIN), jnp.bfloat16)
        copies[:, MARGIN + cells :] = jnp.zeros((planes * fields, MARGIN), jnp.bfloat16)

    @pl.when(step < chunks)
    def _():
        base = pl.multiple_of(step * CHUNK, TILE)
        for plane in range(planes):
            rows = slice(fields * plane, fields * (plane + 1))
            first = partial[plane]
            for offset in range(1, REACH + 1):
                if plane - offset < 0:
                    first = first - half_scale * stencil_coeffs[offset] * below[REACH + plane - offset, :, pl.ds(base, CHUNK)].astype(jnp.float32)
                if plane + offset >= planes:
                    first = first - half_scale * stencil_coeffs[offset] * above[plane + offset - planes, :, pl.ds(base, CHUNK)].astype(jnp.float32)
            firsts[rows, pl.ds(base, CHUNK)] = first
            copies[rows, pl.ds(pl.multiple_of(base + MARGIN, 128), CHUNK)] = first.astype(jnp.bfloat16)

    @pl.when(step > 0)
    def _():
        base = pl.multiple_of((step - 1) * CHUNK, TILE)
        rim = rim_matrix()
        row = lax.broadcasted_iota(jnp.int32, (fields, TILE), 0)
        turn = jnp.where(row < fields // 2, 2.0 * bessel_terms[1], -2.0 * bessel_terms[1])
        for phase in range(CHUNK // TILE):
            start = pl.multiple_of(base + phase * TILE, TILE)
            lanes = slice(phase * TILE, (phase + 1) * TILE)
            in_plane = jnp.dot(copies[:, pl.ds(start, WINDOW)], table[phase % (PERIOD // TILE)], preferred_element_type=jnp.float32)
            origin = [joined(orbitals, plane, lanes) for plane in range(planes)]
            first = [firsts[fields * plane : fields * (plane + 1), pl.ds(start, TILE)] for plane in range(planes)]
            for plane in range(planes):
                rows = slice(fields * plane, fields * (plane + 1))
                energy = (
                    center_factor(potential, plane, lanes) * first[plane]
                    - (half_scale / TABLE_SCALE) * in_plane[rows]
                    - across(lambda at: first[at], plane, planes)
                )
                result = (
                    (bessel_terms[0] + 2.0 * bessel_terms[2]) * origin[plane]
                    + turn * pltpu.roll(first[plane], fields // 2, 0)
                    - (4.0 * bessel_terms[2]) * energy
                )
                gain = 4.0 * bessel_terms[2] * half_scale
                if plane < REACH:
                    total = sum(float(gain * rim[plane, at]) * origin[at] for at in range(REACH))
                    result = result + flags[0] * total
                mirrored = planes - 1 - plane
                if mirrored < REACH:
                    total = sum(float(gain * rim[mirrored, at]) * origin[planes - 1 - at] for at in range(REACH))
                    result = result + flags[1] * total
                out[plane, :, lanes] = result


def second_partial(partial, below, above, moved, potential, table):
    _, planes, count, cells = moved.shape
    chunks = cells // CHUNK
    fields = 2 * count
    ahead = lambda i: jnp.minimum(i, chunks - 1)
    behind = lambda i: jnp.maximum(i - 1, 0)
    rim_spec = pl.BlockSpec(memory_space=pltpu.VMEM)
    return pl.pallas_call(
        second_kernel,
        grid=(chunks + 1,),
        in_specs=[
            pl.BlockSpec((planes, fields, CHUNK), lambda i: (0, 0, ahead(i))),
            rim_spec,
            rim_spec,
            pl.BlockSpec((2, planes, count, CHUNK), lambda i: (0, 0, 0, behind(i))),
            pl.BlockSpec((planes, CHUNK), lambda i: (0, behind(i))),
            pl.BlockSpec(table.shape, lambda i: (0, 0, 0)),
        ],
        out_specs=pl.BlockSpec((planes, fields, CHUNK), lambda i: (0, 0, behind(i))),
        out_shape=jax.ShapeDtypeStruct((planes, fields, cells), jnp.float32),
        scratch_shapes=[
            pltpu.VMEM((planes * fields, cells + 2 * MARGIN), jnp.bfloat16),
            pltpu.VMEM((planes * fields, cells), jnp.float32),
        ],
        cost_estimate=pl.CostEstimate(flops=10**8, transcendentals=0, bytes_accessed=10**7),
        name="second_partial",
    )(partial, below, above, moved, potential, table)


BLOCK = 384
LANES = 128


def halves(values):
    coarse = values.astype(jnp.bfloat16)
    return coarse, (values - coarse.astype(jnp.float32)).astype(jnp.bfloat16)


def exact_product(left, right):
    return jnp.dot(left, right, precision=lax.Precision.HIGHEST, preferred_element_type=jnp.float32)


def product(left, right, contract=0):
    numbers = (((1,), (contract,)), ((), ()))
    dot = lambda a, b: lax.dot_general(a, b, numbers, preferred_element_type=jnp.float32)
    left_coarse, left_rest = halves(left)
    right_coarse, right_rest = halves(right)
    return dot(left_coarse, right_coarse) + (dot(left_coarse, right_rest) + dot(left_rest, right_coarse))


def power_over(peak):
    lift = 14.0 - jnp.floor(jnp.log2(jnp.where(peak > 0.0, peak, 1.0)))
    return jnp.clip(lift, -110.0, 110.0)


def packed(values, lift):
    scaled = values * jnp.exp2(lift)
    lane = lax.broadcasted_iota(jnp.int32, scaled.shape, 1)
    coarse = scaled.astype(jnp.bfloat16).astype(jnp.float32)
    rest = (scaled - coarse)[:, :1]
    scaled = jnp.where(lane == 0, coarse, scaled)
    scaled = jnp.where(lane == NZ, lift, scaled)
    return jnp.where(lane == NZ + 1, rest, scaled)


def unpacked(block):
    lane = lax.broadcasted_iota(jnp.int32, block.shape, 1)
    whole = jnp.where(lane == 0, block + block[:, NZ + 1 : NZ + 2], block)
    return jnp.where(lane < NZ, whole * jnp.exp2(-block[:, NZ : NZ + 1]), 0.0)


def spread_table(block, table):
    table[...] = jnp.zeros(table.shape, table.dtype)
    for part in range(BLOCK // NZ):
        table[part * NZ : (part + 1) * NZ, part * LANES : (part + 1) * LANES] = block[...]


def finish_kernel(shares, partial, below, above, z_block, y_table, out, chunks, z_table, rows, along_z, along_y, sent):
    planes = partial.shape[0]
    fields = partial.shape[1]
    count = fields // 2
    groups = rows.shape[0]
    members = chunks.shape[0]
    step = pl.program_id(0)
    per_step = WIDE_CHUNK // BLOCK
    lanes = pl.ds(pl.multiple_of(step * WIDE_CHUNK, LANES), WIDE_CHUNK)
    gain = 4.0 * bessel_terms[2] * 0.5 / energy_scale
    field = lax.broadcasted_iota(jnp.int32, (fields, 1), 0) % count
    weight = jnp.zeros((fields, 1), jnp.float32)
    for at in range(count):
        weight = jnp.where(field == at, shares[at], weight)
    weight = weight * (1.0 / (count * lax.axis_size("band")))
    for plane in range(planes):
        value = partial[plane]
        if plane < REACH:
            value = value + gain * below[plane, :, lanes].astype(jnp.float32)
        if planes - 1 - plane < REACH:
            value = value + gain * above[planes - 1 - plane, :, lanes].astype(jnp.float32)
        out[0, plane] = value[:count]
        out[1, plane] = value[count:]
        total = jnp.sum(weight * (value * value), axis=0, keepdims=True)
        for group in range(per_step):
            rows[step * per_step + group, plane : plane + 1, :] = total[:, group * BLOCK : (group + 1) * BLOCK]

    @pl.when(step == pl.num_programs(0) - 1)
    def _():
        padded = rows.shape[1]
        spread_table(z_block, z_table)
        turned = product(rows[...].reshape(groups * padded, BLOCK), z_table[...])
        for part in range(BLOCK // NZ):
            along_z[part] = turned[:, part * LANES : (part + 1) * LANES]
        for plane in range(planes):
            for part in range(BLOCK // NZ):
                along_y[part * groups : (part + 1) * groups, plane * LANES : (plane + 1) * LANES] = along_z[
                    part, pl.ds(plane, groups, stride=padded), :
                ]
        waves = product(y_table[...], along_y[...])
        peak = jnp.max(jnp.max(jnp.abs(waves), axis=1, keepdims=True), axis=0, keepdims=True)
        lift = power_over(peak)
        for part in range(chunks.shape[3] // LANES):
            for plane in range(planes):
                block = waves[part * members : (part + 1) * members, plane * LANES : (plane + 1) * LANES]
                sent[part, pl.ds(plane, members, stride=planes), :] = packed(block, lift)
        for member in range(members):
            for quarter in range(planes // 4):
                start = member * planes + quarter * 4
                for part in range(chunks.shape[3] // LANES):
                    tile = slice(part * LANES, (part + 1) * LANES)
                    chunks[member, quarter, :, tile] = sent[part, start : start + 4, :]


def finish(partial, below, above, occupations, z_table, y_table, members):
    planes, fields, cells = partial.shape
    rim_spec = pl.BlockSpec(memory_space=pltpu.VMEM)
    groups = cells // BLOCK
    padded = -(-planes // 8) * 8
    width = NY // members * LANES
    whole = lambda shape: pl.BlockSpec(shape, lambda i: (0,) * len(shape))
    wave_shape = (members, planes // 4, 4, width)
    return pl.pallas_call(
        finish_kernel,
        grid=(cells // WIDE_CHUNK,),
        in_specs=[
            pl.BlockSpec(memory_space=pltpu.SMEM),
            pl.BlockSpec((planes, fields, WIDE_CHUNK), lambda i: (0, 0, i)),
            rim_spec,
            rim_spec,
            whole(z_table.shape),
            whole(y_table.shape),
        ],
        out_specs=[pl.BlockSpec((2, planes, fields // 2, WIDE_CHUNK), lambda i: (0, 0, 0, i)), pl.BlockSpec(memory_space=pltpu.VMEM)],
        out_shape=[
            jax.ShapeDtypeStruct((2, planes, fields // 2, cells), jnp.float32),
            pltpu.VMEM(wave_shape, jnp.float32),
        ],
        scratch_shapes=[
            pltpu.VMEM((BLOCK, BLOCK // NZ * LANES), jnp.float32),
            pltpu.VMEM((groups, padded, BLOCK), jnp.float32),
            pltpu.VMEM((BLOCK // NZ, groups * padded, LANES), jnp.float32),
            pltpu.VMEM((NY, planes * LANES), jnp.float32),
            pltpu.VMEM((width // LANES, members * planes, LANES), jnp.float32),
        ],
        name="finish",
    )(occupations, partial, below, above, z_table, y_table)


def column_kernel(arrived, multiplier, x_table, back_table, chunks, raw, columns, both):
    members, quarters, _, width = arrived.shape
    planes = quarters * 4
    blocks = chunks.shape[0]
    length = blocks * planes
    for member in range(members):
        for quarter in range(quarters):
            start = member * planes + quarter * 4
            raw[start : start + 4, :] = arrived[member, quarter]
    for part in range(width // LANES):
        lanes = slice(part * LANES, (part + 1) * LANES)
        total = unpacked(raw[:length, lanes])
        for band in range(1, members // blocks):
            total = total + unpacked(raw[band * length : (band + 1) * length, lanes])
        columns[:, lanes] = total
    waves = exact_product(x_table[...], columns[...]) * multiplier[...]
    field = exact_product(back_table[...], waves)
    for index, values in enumerate((columns[...], field)):
        peak = jnp.max(jnp.max(jnp.abs(values), axis=1, keepdims=True), axis=0, keepdims=True)
        lift = power_over(peak)
        for part in range(width // LANES):
            at = index * width + part * LANES
            both[:, at : at + LANES] = packed(values[:, part * LANES : (part + 1) * LANES], lift)
    for block in range(blocks):
        for quarter in range(quarters):
            start = block * planes + quarter * 4
            chunks[block, quarter] = both[start : start + 4, :]


def column_waves(arrived, multiplier, x_table, blocks):
    members, quarters, _, width = arrived.shape
    length = x_table.shape[0]
    return pl.pallas_call(
        column_kernel,
        out_shape=pltpu.VMEM((blocks, quarters, 4, 2 * width), jnp.float32),
        out_specs=pl.BlockSpec(memory_space=pltpu.VMEM),
        scratch_shapes=[
            pltpu.VMEM((members * quarters * 4, width), jnp.float32),
            pltpu.VMEM((length, width), jnp.float32),
            pltpu.VMEM((length, 2 * width), jnp.float32),
        ],
        name="column_waves",
    )(arrived, multiplier, jnp.asarray(x_table), jnp.asarray(x_table.T))


def return_kernel(arrived, y_back, z_block, density, hartree, z_table, raw, along_y, along_z, result):
    members, quarters, _, width = arrived.shape
    width //= 2
    planes = quarters * 4
    groups = result.shape[1] // planes
    spread_table(z_block, z_table)
    for member in range(members):
        for quarter in range(quarters):
            start = member * planes + quarter * 4
            for part in range(2 * width // LANES):
                raw[part, start : start + 4, :] = arrived[member, quarter, :, part * LANES : (part + 1) * LANES]
    for index, out in enumerate((density, hartree)):
        for plane in range(planes):
            for part in range(width // LANES):
                block = raw[index * (width // LANES) + part, pl.ds(plane, members, stride=planes), :]
                along_y[part * members : (part + 1) * members, plane * LANES : (plane + 1) * LANES] = unpacked(block)
        waves = product(y_back[...], along_y[...])
        for plane in range(planes):
            for part in range(BLOCK // NZ):
                along_z[plane * groups : (plane + 1) * groups, part * LANES : (part + 1) * LANES] = waves[
                    part * groups : (part + 1) * groups, plane * LANES : (plane + 1) * LANES
                ]
        cells = product(along_z[...], z_table[...], 1)
        for tile in range(BLOCK // LANES):
            result[tile] = cells[:, tile * LANES : (tile + 1) * LANES]
        for group in range(groups):
            for tile in range(BLOCK // LANES):
                at = group * BLOCK + tile * LANES
                out[:, at : at + LANES] = result[tile, pl.ds(group, planes, stride=groups), :]


def return_waves(arrived, y_table, z_table, cells):
    members, quarters, _, width = arrived.shape
    planes = quarters * 4
    groups = cells // BLOCK
    plane_shape = jax.ShapeDtypeStruct((planes, cells), jnp.float32)
    return pl.pallas_call(
        return_kernel,
        out_shape=[plane_shape, plane_shape],
        scratch_shapes=[
            pltpu.VMEM((BLOCK, BLOCK // NZ * LANES), jnp.float32),
            pltpu.VMEM((width // LANES, members * planes, LANES), jnp.float32),
            pltpu.VMEM((NY, planes * LANES), jnp.float32),
            pltpu.VMEM((planes * groups, BLOCK // NZ * LANES), jnp.float32),
            pltpu.VMEM((BLOCK // LANES, planes * groups, LANES), jnp.float32),
        ],
        name="return_waves",
    )(arrived, y_table, z_table)


def wave_basis(length):
    cells = np.arange(length)
    rows = []
    waves = []
    for wave in range(length // 2 + 1):
        norm = math.sqrt((1.0 if wave in (0, length / 2) else 2.0) / length)
        rows.append(norm * np.cos(2.0 * math.pi / length * (wave * cells % length)))
        waves.append(wave)
    for wave in range(1, (length + 1) // 2):
        rows.append(math.sqrt(2.0 / length) * np.sin(2.0 * math.pi / length * (wave * cells % length)))
        waves.append(wave)
    return np.asarray(rows, np.float32), (2.0 * math.pi / length * np.asarray(waves, np.float64)) ** 2


def wave_tables(members, length):
    z_basis, z_squares = wave_basis(NZ)
    y_basis, y_squares = wave_basis(NY)
    x_basis, x_squares = wave_basis(length)
    parts = BLOCK // NZ
    z_table = np.pad(z_basis.T, ((0, 0), (0, LANES - NZ)))
    rows = NY // members
    y_table = y_basis.reshape(members, rows, NY // parts, parts).transpose(1, 0, 3, 2).reshape(NY, NY)
    return z_table, y_table, x_basis, (x_squares, y_squares, z_squares)


def density_and_field(waves, tables, cells):
    bands = lax.axis_size("band")
    blocks = lax.axis_size("space")
    members, quarters, _, width = waves.shape
    z_table, y_table, x_table, (x_squares, y_squares, z_squares) = tables
    exchange = lambda chunks: lax.all_to_all(
        chunks.astype(jnp.float16), ("band", "space"), split_axis=0, concat_axis=0, tiled=True
    ).astype(jnp.float32)
    rows = NY // members
    place = (lax.axis_index("band") * blocks + lax.axis_index("space")) * rows
    squares = (
        jnp.asarray(x_squares, jnp.float32)[:, None, None]
        + lax.dynamic_slice_in_dim(jnp.asarray(y_squares, jnp.float32), place, rows)[None, :, None]
        + jnp.asarray(np.pad(z_squares, (0, LANES - NZ)), jnp.float32)[None, None, :]
    )
    used = lax.broadcasted_iota(jnp.int32, squares.shape, 2) < NZ
    multiplier = jnp.where(
        (squares > 0) & used, 4.0 * math.pi / jnp.where(squares > 0, squares, 1.0), 0.0
    ).reshape(-1, width)
    both = column_waves(exchange(waves), multiplier, x_table, blocks)
    spread = jnp.broadcast_to(both.astype(jnp.float16)[None], (bands, *both.shape)).reshape(members, *both.shape[1:])
    return return_waves(exchange(spread), jnp.asarray(y_table.T), jnp.asarray(z_table), cells)


def in_place(x):
    return pltpu.with_memory_space_constraint(x, pltpu.VMEM)


def per_device_blocks(orbitals, potential, occupations):
    moved = orbitals.transpose(0, 2, 1, 3)
    table = plane_table()
    lower, upper = rim_copies(moved)
    below = in_place(from_behind(upper, "space", 1))
    above = in_place(from_behind(lower, "space", -1))
    partial, to_lower, to_upper = first_partial(moved, potential, table)
    terms_below = in_place(from_behind(to_upper, "space", 1))
    terms_above = in_place(from_behind(to_lower, "space", -1))
    partial = second_partial(partial, below, above, moved, potential, table)
    members = lax.axis_size("band") * lax.axis_size("space")
    tables = wave_tables(members, orbitals.shape[2] * lax.axis_size("space"))
    propagated, waves = finish(
        partial, terms_below, terms_above, occupations, jnp.asarray(tables[0]), jnp.asarray(tables[1]), members
    )
    density, hartree = density_and_field(waves, tables, orbitals.shape[3])
    return (propagated.transpose(0, 2, 1, 3), density, hartree)


def per_device(orbitals, potential, occupations):
    _, count, planes, cells = orbitals.shape
    columns = NY % (lax.axis_size("space") * lax.axis_size("band"))
    if planes < 2 * REACH or planes % 4 or count != 4 or cells % CHUNK or cells % WIDE_CHUNK or PERIOD % NZ or MARGIN != REACH * NZ or columns:
        return per_device_general(orbitals, potential, occupations)
    return per_device_blocks(orbitals, potential, occupations)


def solution(mesh):
    in_specs = (P(None, "band", "space", None), P("space", None), P("band"))
    out_specs = (P(None, "band", "space", None), P("space", None), P("space", None))
    return jax.shard_map(
        per_device, mesh=mesh, in_specs=in_specs, out_specs=out_specs, check_vma=False
    )
```

```python
import math

import jax
import jax.numpy as jnp
import numpy as np
from jax import lax
from jax.experimental import pallas as pl
from jax.experimental.pallas import tpu as pltpu
from jax.sharding import PartitionSpec as P

NX = 96
NY = 96
NZ = 96


stencil_coeffs = (-205.0 / 72.0, 8.0 / 5.0, -1.0 / 5.0, 8.0 / 315.0, -1.0 / 560.0)
energy_shift = 6.0
energy_scale = 8.0
bessel_terms = (0.7651976865579666, 0.44005058574493355, 0.11490348493190049)


def from_behind(x, axis, by):
    count = lax.axis_size(axis)
    pairs = [(i, i + by) for i in range(count) if 0 <= i + by < count]
    return lax.ppermute(x, axis, pairs)


def plane_laplace(center, wider):
    reach_cells = len(stencil_coeffs) - 1
    planes = center.shape[-2]
    cells = center.shape[-1]
    spread = wider.astype(jnp.float32)
    middle = spread[..., reach_cells : reach_cells + planes, :]
    summed = 3.0 * stencil_coeffs[0] * center
    for offset in range(1, reach_cells + 1):
        after = spread[..., reach_cells + offset : reach_cells + offset + planes, :]
        before = spread[..., reach_cells - offset : reach_cells - offset + planes, :]
        summed = summed + stencil_coeffs[offset] * (after + before)
    margin = reach_cells * NZ
    padded = jnp.pad(middle, [(0, 0)] * (middle.ndim - 1) + [(margin, margin)])
    z_index = lax.iota(jnp.int32, cells) % NZ
    for offset in range(1, reach_cells + 1):
        stride = offset * NZ
        beyond = padded[..., margin + stride : margin + stride + cells]
        behind = padded[..., margin - stride : margin - stride + cells]
        summed = summed + stencil_coeffs[offset] * (beyond + behind)
        beyond = jnp.where(
            z_index + offset < NZ, padded[..., margin + offset : margin + offset + cells], 0.0
        )
        behind = jnp.where(
            z_index - offset >= 0, padded[..., margin - offset : margin - offset + cells], 0.0
        )
        summed = summed + stencil_coeffs[offset] * (beyond + behind)
    return summed


def scaled_hamiltonian(center, wider, field_values):
    energy = -0.5 * plane_laplace(center, wider) + field_values * center
    return (energy - energy_shift * center) / energy_scale


def slab_rims(source, extent):
    planes = source.shape[-2]
    lower_parts = []
    upper_parts = []
    for distance in range(1, -(-extent // planes) + 1):
        needed = min(planes, extent - (distance - 1) * planes)
        for heading in (1, -1):
            if heading == 1:
                outgoing = source[..., planes - needed :, :]
            else:
                outgoing = source[..., :needed, :]
            arrived = from_behind(outgoing, "space", heading * distance)
            if heading == 1:
                lower_parts.append(arrived)
            else:
                upper_parts.append(arrived)
    return jnp.concatenate(lower_parts[::-1] + [source] + upper_parts, axis=-2)


def dft_tables(length):
    indices = lax.iota(jnp.int32, length)
    product = indices[:, None] * indices[None, :] % length
    phases = 2.0 * math.pi / length * product.astype(jnp.float32)
    return (jnp.cos(phases), jnp.sin(phases))


def turn_axis(cosine, sines, values, pattern):
    direct = jnp.einsum(pattern, cosine, values, precision=lax.Precision.HIGHEST)
    crossed = jnp.einsum(pattern, sines, values, precision=lax.Precision.HIGHEST)
    real_part = direct[..., :NZ] - crossed[..., NZ:]
    imag_part = direct[..., NZ:] + crossed[..., :NZ]
    return jnp.concatenate([real_part, imag_part], axis=-1)


def squared_waves(length, anchor, extent):
    indices = anchor + lax.iota(jnp.int32, extent)
    signed = jnp.where(indices < (length + 1) // 2, indices, indices - length).astype(jnp.float32)
    return (2.0 * math.pi / length * signed) ** 2


def hartree_field(density):
    planes = density.shape[0]
    z_cosine, z_sine = dft_tables(NZ)
    y_cosine, y_sine = dft_tables(NY)
    x_cosine, x_sine = dft_tables(NX)
    forward_z = jnp.concatenate([z_cosine, -z_sine], axis=1)
    flattened = density.reshape(planes * NY, NZ)
    spectral = jnp.dot(
        flattened, forward_z, precision=lax.Precision.HIGHEST, preferred_element_type=jnp.float32
    )
    spectral = turn_axis(y_cosine, -y_sine, spectral.reshape(planes, NY, 2 * NZ), "ky,xyz->xkz")
    columns = lax.all_to_all(spectral, "space", split_axis=1, concat_axis=0, tiled=True)
    y_rows = columns.shape[1]
    spectral = turn_axis(x_cosine, -x_sine, columns, "kx,xyz->kyz")
    squares = (
        squared_waves(NX, 0, NX)[:, None, None]
        + squared_waves(NY, lax.axis_index("space") * y_rows, y_rows)[None, :, None]
        + squared_waves(NZ, 0, NZ)[None, None, :]
    )
    kernel = jnp.where(squares > 0, 4.0 * math.pi / jnp.where(squares > 0, squares, 1.0), 0.0)
    spectral = spectral * jnp.concatenate([kernel, kernel], axis=-1)
    spectral = turn_axis(x_cosine, x_sine, spectral, "kx,xyz->kyz")
    slabs = lax.all_to_all(spectral, "space", split_axis=0, concat_axis=1, tiled=True)
    spectral = turn_axis(y_cosine, y_sine, slabs, "ky,xyz->xkz")
    inverse_z = jnp.concatenate([z_cosine, -z_sine], axis=0)
    field_values = jnp.dot(
        spectral.reshape(planes * NY, 2 * NZ),
        inverse_z,
        precision=lax.Precision.HIGHEST,
        preferred_element_type=jnp.float32,
    )
    return (field_values / (NX * NY * NZ)).reshape(planes, NY * NZ)


def per_device_general(orbitals, potential, occupations):
    reach_cells = len(stencil_coeffs) - 1
    orbital_count = orbitals.shape[1]
    zero_copy = slab_rims(orbitals.astype(jnp.bfloat16), reach_cells)
    first_term = scaled_hamiltonian(orbitals, zero_copy, potential)
    first_copy = slab_rims(first_term.astype(jnp.bfloat16), reach_cells)
    second_term = 2.0 * scaled_hamiltonian(first_term, first_copy, potential) - orbitals
    prop_real = (
        bessel_terms[0] * orbitals[0]
        + 2.0 * bessel_terms[1] * first_term[1]
        - 2.0 * bessel_terms[2] * second_term[0]
    )
    prop_imag = (
        bessel_terms[0] * orbitals[1]
        - 2.0 * bessel_terms[1] * first_term[0]
        - 2.0 * bessel_terms[2] * second_term[1]
    )
    propagated = jnp.stack([prop_real, prop_imag])
    weights = occupations / (orbital_count * lax.axis_size("band"))
    partial_density = jnp.sum(
        weights[:, None, None] * (prop_real * prop_real + prop_imag * prop_imag), axis=0
    )
    density = lax.psum(partial_density, "band")
    hartree = hartree_field(density)
    return (propagated, density, hartree)


REACH = len(stencil_coeffs) - 1
TABLE_SCALE = 5040.0
PERIOD = 768
CHUNK = 2304
WIDE_CHUNK = 4608
KERNEL_MEMORY = 36 * 2**20
WINDOW = 1024
TILE = 256
MARGIN = 384


def plane_table():
    phases = PERIOD // TILE
    table = np.zeros((phases, WINDOW, TILE), np.float32)
    scaled = [round(coeff * TABLE_SCALE) for coeff in stencil_coeffs[1:]]
    for phase in range(phases):
        target = phase * TILE + np.arange(TILE)[None, :]
        origin = phase * TILE - MARGIN + np.arange(WINDOW)[:, None]
        y_step = origin // NZ - target // NZ
        z_step = origin % NZ - target % NZ
        for offset in range(1, REACH + 1):
            along_y = (np.abs(y_step) == offset) & (z_step == 0)
            along_z = (y_step == 0) & (np.abs(z_step) == offset)
            table[phase] += scaled[offset - 1] * (along_y | along_z)
    return jnp.asarray(table, jnp.bfloat16)


def joined(block, plane, lanes=slice(None)):
    return jnp.concatenate([block[0, plane, :, lanes], block[1, plane, :, lanes]], axis=0)


def rim_kernel(orbitals, lower, upper, staged, arrivals):
    planes = orbitals.shape[1]
    starts = (0, planes - REACH)
    copies = [
        pltpu.make_async_copy(orbitals.at[:, pl.ds(start, REACH)], staged.at[side], arrivals.at[side])
        for side, start in enumerate(starts)
    ]
    for copy in copies:
        copy.start()
    for side, rim in enumerate((lower, upper)):
        copies[side].wait()
        for plane in range(REACH):
            rim[plane] = jnp.concatenate([staged[side, 0, plane], staged[side, 1, plane]], axis=0).astype(jnp.bfloat16)


def rim_copies(moved):
    _, planes, count, cells = moved.shape
    rim = pltpu.VMEM((REACH, 2 * count, cells), jnp.bfloat16)
    return pl.pallas_call(
        rim_kernel,
        in_specs=[pl.BlockSpec(memory_space=pl.ANY)],
        out_specs=[pl.BlockSpec(memory_space=pltpu.VMEM)] * 2,
        out_shape=[rim, rim],
        scratch_shapes=[
            pltpu.VMEM((2, 2, REACH, count, cells), jnp.float32),
            pltpu.SemaphoreType.DMA((2,)),
        ],
        compiler_params=pltpu.CompilerParams(vmem_limit_bytes=KERNEL_MEMORY),
        name="rim_copies",
    )(moved)


def center_factor(potential, plane, lanes):
    shift = energy_shift + 1.5 * stencil_coeffs[0]
    return (potential[plane : plane + 1, lanes] - shift) * (1.0 / energy_scale)


def across(values, plane, planes):
    total = None
    for offset in range(1, REACH + 1):
        pair = [values(at) for at in (plane - offset, plane + offset) if 0 <= at < planes]
        if pair:
            both = pair[0] + pair[1] if len(pair) == 2 else pair[0]
            term = (0.5 / energy_scale * stencil_coeffs[offset]) * both
            total = term if total is None else total + term
    return total


def first_kernel(current, left, right, potential, table, partial, to_lower, to_upper, copies, values):
    planes = current.shape[1]
    fields = 2 * current.shape[2]
    step = pl.program_id(0)
    last = pl.num_programs(0) - 1
    for plane in range(planes):
        rows = slice(fields * plane, fields * (plane + 1))
        own = joined(current, plane)
        values[rows, :] = own
        copies[rows, MARGIN : MARGIN + CHUNK] = own.astype(jnp.bfloat16)
        before = joined(left, plane)
        after = joined(right, plane)
        copies[rows, :MARGIN] = jnp.where(step == 0, 0.0, before).astype(jnp.bfloat16)
        copies[rows, MARGIN + CHUNK :] = jnp.where(step == last, 0.0, after).astype(jnp.bfloat16)
    for phase in range(CHUNK // TILE):
        lanes = slice(phase * TILE, (phase + 1) * TILE)
        in_plane = jnp.dot(
            copies[:, phase * TILE : phase * TILE + WINDOW], table[phase % (PERIOD // TILE)], preferred_element_type=jnp.float32
        )
        results = []
        for plane in range(planes):
            rows = slice(fields * plane, fields * (plane + 1))
            result = (
                center_factor(potential, plane, lanes) * values[rows, lanes]
                - (0.5 / energy_scale / TABLE_SCALE) * in_plane[rows]
                - across(lambda at: values[fields * at : fields * (at + 1), lanes], plane, planes)
            )
            partial[plane, :, pl.ds(pl.multiple_of(step * CHUNK + phase * TILE, TILE), TILE)] = result
            results.append(result)
        for rim, into, order in ((to_upper, "up", results[::-1]), (to_lower, "down", results)):
            for plane in range(REACH):
                total = None
                for offset in range(plane + 1, REACH + 1):
                    term = stencil_coeffs[offset] * order[offset - plane - 1]
                    total = term if total is None else total + term
                rim[plane, :, pl.ds(pl.multiple_of(step * CHUNK + phase * TILE, TILE), TILE)] = total.astype(jnp.bfloat16)


def first_partial(moved, potential, table):
    _, planes, count, cells = moved.shape
    chunks = cells // CHUNK
    margins = CHUNK // MARGIN
    fields = 2 * count
    rim = pltpu.VMEM((REACH, fields, cells), jnp.bfloat16)
    rim_spec = pl.BlockSpec(memory_space=pltpu.VMEM)
    return pl.pallas_call(
        first_kernel,
        grid=(chunks,),
        in_specs=[
            pl.BlockSpec((2, planes, count, CHUNK), lambda i: (0, 0, 0, i)),
            pl.BlockSpec((2, planes, count, MARGIN), lambda i: (0, 0, 0, jnp.maximum(margins * i - 1, 0))),
            pl.BlockSpec(
                (2, planes, count, MARGIN),
                lambda i: (0, 0, 0, jnp.minimum(margins * (i + 1), margins * chunks - 1)),
            ),
            pl.BlockSpec((planes, CHUNK), lambda i: (0, i)),
            pl.BlockSpec(table.shape, lambda i: (0, 0, 0)),
        ],
        out_specs=[rim_spec, rim_spec, rim_spec],
        out_shape=[pltpu.VMEM((planes, fields, cells), jnp.float32), rim, rim],
        scratch_shapes=[
            pltpu.VMEM((planes * fields, CHUNK + 2 * MARGIN), jnp.bfloat16),
            pltpu.VMEM((planes * fields, CHUNK), jnp.float32),
        ],
        cost_estimate=pl.CostEstimate(flops=10**8, transcendentals=0, bytes_accessed=10**7),
        compiler_params=pltpu.CompilerParams(vmem_limit_bytes=KERNEL_MEMORY),
        name="first_partial",
    )(moved, moved, moved, potential, table)


def rim_matrix():
    coeffs = stencil_coeffs
    matrix = np.zeros((REACH, REACH))
    for plane in range(REACH):
        for origin in range(REACH):
            for beyond in range(1, REACH + 1):
                if plane + beyond <= REACH and origin + beyond <= REACH:
                    matrix[plane, origin] -= 0.5 / energy_scale * coeffs[plane + beyond] * coeffs[origin + beyond]
    return matrix


def second_kernel(partial, below, above, orbitals, potential, table, out, copies, firsts):
    planes = partial.shape[0]
    fields = partial.shape[1]
    cells = firsts.shape[1]
    step = pl.program_id(0)
    chunks = pl.num_programs(0) - 1
    half_scale = 0.5 / energy_scale
    place = lax.axis_index("space")
    flags = [(place > 0).astype(jnp.float32), (place < lax.axis_size("space") - 1).astype(jnp.float32)]

    @pl.when(step == 0)
    def _():
        copies[:, :MARGIN] = jnp.zeros((planes * fields, MARGIN), jnp.bfloat16)
        copies[:, MARGIN + cells :] = jnp.zeros((planes * fields, MARGIN), jnp.bfloat16)

    @pl.when(step < chunks)
    def _():
        base = pl.multiple_of(step * CHUNK, TILE)
        for plane in range(planes):
            rows = slice(fields * plane, fields * (plane + 1))
            first = partial[plane, :, pl.ds(base, CHUNK)]
            for offset in range(1, REACH + 1):
                if plane - offset < 0:
                    first = first - half_scale * stencil_coeffs[offset] * below[REACH + plane - offset, :, pl.ds(base, CHUNK)].astype(jnp.float32)
                if plane + offset >= planes:
                    first = first - half_scale * stencil_coeffs[offset] * above[plane + offset - planes, :, pl.ds(base, CHUNK)].astype(jnp.float32)
            firsts[rows, pl.ds(base, CHUNK)] = first
            copies[rows, pl.ds(pl.multiple_of(base + MARGIN, 128), CHUNK)] = first.astype(jnp.bfloat16)

    @pl.when(step > 0)
    def _():
        base = pl.multiple_of((step - 1) * CHUNK, TILE)
        rim = rim_matrix()
        row = lax.broadcasted_iota(jnp.int32, (fields, TILE), 0)
        turn = jnp.where(row < fields // 2, 2.0 * bessel_terms[1], -2.0 * bessel_terms[1])
        for phase in range(CHUNK // TILE):
            start = pl.multiple_of(base + phase * TILE, TILE)
            lanes = slice(phase * TILE, (phase + 1) * TILE)
            in_plane = jnp.dot(copies[:, pl.ds(start, WINDOW)], table[phase % (PERIOD // TILE)], preferred_element_type=jnp.float32)
            origin = [joined(orbitals, plane, lanes) for plane in range(planes)]
            first = [firsts[fields * plane : fields * (plane + 1), pl.ds(start, TILE)] for plane in range(planes)]
            for plane in range(planes):
                rows = slice(fields * plane, fields * (plane + 1))
                energy = (
                    center_factor(potential, plane, lanes) * first[plane]
                    - (half_scale / TABLE_SCALE) * in_plane[rows]
                    - across(lambda at: first[at], plane, planes)
                )
                result = (
                    (bessel_terms[0] + 2.0 * bessel_terms[2]) * origin[plane]
                    + turn * pltpu.roll(first[plane], fields // 2, 0)
                    - (4.0 * bessel_terms[2]) * energy
                )
                gain = 4.0 * bessel_terms[2] * half_scale
                if plane < REACH:
                    total = sum(float(gain * rim[plane, at]) * origin[at] for at in range(REACH))
                    result = result + flags[0] * total
                mirrored = planes - 1 - plane
                if mirrored < REACH:
                    total = sum(float(gain * rim[mirrored, at]) * origin[planes - 1 - at] for at in range(REACH))
                    result = result + flags[1] * total
                out[plane, :, pl.ds(start, TILE)] = result


def second_partial(partial, below, above, moved, potential, table):
    _, planes, count, cells = moved.shape
    chunks = cells // CHUNK
    fields = 2 * count
    ahead = lambda i: jnp.minimum(i, chunks - 1)
    behind = lambda i: jnp.maximum(i - 1, 0)
    rim_spec = pl.BlockSpec(memory_space=pltpu.VMEM)
    return pl.pallas_call(
        second_kernel,
        grid=(chunks + 1,),
        in_specs=[
            rim_spec,
            rim_spec,
            rim_spec,
            pl.BlockSpec((2, planes, count, CHUNK), lambda i: (0, 0, 0, behind(i))),
            pl.BlockSpec((planes, CHUNK), lambda i: (0, behind(i))),
            pl.BlockSpec(table.shape, lambda i: (0, 0, 0)),
        ],
        out_specs=rim_spec,
        out_shape=pltpu.VMEM((planes, fields, cells), jnp.float32),
        scratch_shapes=[
            pltpu.VMEM((planes * fields, cells + 2 * MARGIN), jnp.bfloat16),
            pltpu.VMEM((planes * fields, cells), jnp.float32),
        ],
        cost_estimate=pl.CostEstimate(flops=10**8, transcendentals=0, bytes_accessed=10**7),
        compiler_params=pltpu.CompilerParams(vmem_limit_bytes=KERNEL_MEMORY),
        name="second_partial",
    )(partial, below, above, moved, potential, table)


BLOCK = 384
LANES = 128


def halves(values):
    coarse = values.astype(jnp.bfloat16)
    return coarse, (values - coarse.astype(jnp.float32)).astype(jnp.bfloat16)


def exact_product(left, right):
    return jnp.dot(left, right, precision=lax.Precision.HIGHEST, preferred_element_type=jnp.float32)


def product(left, right, contract=0):
    numbers = (((1,), (contract,)), ((), ()))
    dot = lambda a, b: lax.dot_general(a, b, numbers, preferred_element_type=jnp.float32)
    left_coarse, left_rest = halves(left)
    right_coarse, right_rest = halves(right)
    return dot(left_coarse, right_coarse) + (dot(left_coarse, right_rest) + dot(left_rest, right_coarse))


def power_over(peak):
    lift = 14.0 - jnp.floor(jnp.log2(jnp.where(peak > 0.0, peak, 1.0)))
    return jnp.clip(lift, -110.0, 110.0)


def packed(values, lift):
    scaled = values * jnp.exp2(lift)
    lane = lax.broadcasted_iota(jnp.int32, scaled.shape, 1)
    coarse = scaled.astype(jnp.bfloat16).astype(jnp.float32)
    rest = (scaled - coarse)[:, :1]
    scaled = jnp.where(lane == 0, coarse, scaled)
    scaled = jnp.where(lane == NZ, lift, scaled)
    return jnp.where(lane == NZ + 1, rest, scaled)


def unpacked(block):
    lane = lax.broadcasted_iota(jnp.int32, block.shape, 1)
    whole = jnp.where(lane == 0, block + block[:, NZ + 1 : NZ + 2], block)
    return jnp.where(lane < NZ, whole * jnp.exp2(-block[:, NZ : NZ + 1]), 0.0)


def spread_table(block, table):
    table[...] = jnp.zeros(table.shape, table.dtype)
    for part in range(BLOCK // NZ):
        table[part * NZ : (part + 1) * NZ, part * LANES : (part + 1) * LANES] = block[...]


def finish_kernel(shares, partial, below, above, z_block, y_table, out, chunks, z_table, rows, along_z, along_y, sent):
    planes = partial.shape[0]
    fields = partial.shape[1]
    count = fields // 2
    groups = rows.shape[0]
    members = chunks.shape[0]
    step = pl.program_id(0)
    per_step = WIDE_CHUNK // BLOCK
    lanes = pl.ds(pl.multiple_of(step * WIDE_CHUNK, LANES), WIDE_CHUNK)
    gain = 4.0 * bessel_terms[2] * 0.5 / energy_scale
    field = lax.broadcasted_iota(jnp.int32, (fields, 1), 0) % count
    weight = jnp.zeros((fields, 1), jnp.float32)
    for at in range(count):
        weight = jnp.where(field == at, shares[at], weight)
    weight = weight * (1.0 / (count * lax.axis_size("band")))
    for plane in range(planes):
        value = partial[plane, :, lanes]
        if plane < REACH:
            value = value + gain * below[plane, :, lanes].astype(jnp.float32)
        if planes - 1 - plane < REACH:
            value = value + gain * above[planes - 1 - plane, :, lanes].astype(jnp.float32)
        out[0, plane] = value[:count]
        out[1, plane] = value[count:]
        total = jnp.sum(weight * (value * value), axis=0, keepdims=True)
        for group in range(per_step):
            rows[step * per_step + group, plane : plane + 1, :] = total[:, group * BLOCK : (group + 1) * BLOCK]

    @pl.when(step == pl.num_programs(0) - 1)
    def _():
        padded = rows.shape[1]
        spread_table(z_block, z_table)
        turned = product(rows[...].reshape(groups * padded, BLOCK), z_table[...])
        for part in range(BLOCK // NZ):
            along_z[part] = turned[:, part * LANES : (part + 1) * LANES]
        for plane in range(planes):
            for part in range(BLOCK // NZ):
                along_y[part * groups : (part + 1) * groups, plane * LANES : (plane + 1) * LANES] = along_z[
                    part, pl.ds(plane, groups, stride=padded), :
                ]
        waves = product(y_table[...], along_y[...])
        peak = jnp.max(jnp.max(jnp.abs(waves), axis=1, keepdims=True), axis=0, keepdims=True)
        lift = power_over(peak)
        for part in range(chunks.shape[3] // LANES):
            for plane in range(planes):
                block = waves[part * members : (part + 1) * members, plane * LANES : (plane + 1) * LANES]
                sent[part, pl.ds(plane, members, stride=planes), :] = packed(block, lift)
        for member in range(members):
            for quarter in range(planes // 4):
                start = member * planes + quarter * 4
                for part in range(chunks.shape[3] // LANES):
                    tile = slice(part * LANES, (part + 1) * LANES)
                    chunks[member, quarter, :, tile] = sent[part, start : start + 4, :]


def finish(partial, below, above, occupations, z_table, y_table, members):
    planes, fields, cells = partial.shape
    rim_spec = pl.BlockSpec(memory_space=pltpu.VMEM)
    groups = cells // BLOCK
    padded = -(-planes // 8) * 8
    width = NY // members * LANES
    whole = lambda shape: pl.BlockSpec(shape, lambda i: (0,) * len(shape))
    wave_shape = (members, planes // 4, 4, width)
    return pl.pallas_call(
        finish_kernel,
        grid=(cells // WIDE_CHUNK,),
        in_specs=[
            pl.BlockSpec(memory_space=pltpu.SMEM),
            rim_spec,
            rim_spec,
            rim_spec,
            whole(z_table.shape),
            whole(y_table.shape),
        ],
        out_specs=[pl.BlockSpec((2, planes, fields // 2, WIDE_CHUNK), lambda i: (0, 0, 0, i)), pl.BlockSpec(memory_space=pltpu.VMEM)],
        out_shape=[
            jax.ShapeDtypeStruct((2, planes, fields // 2, cells), jnp.float32),
            pltpu.VMEM(wave_shape, jnp.float32),
        ],
        scratch_shapes=[
            pltpu.VMEM((BLOCK, BLOCK // NZ * LANES), jnp.float32),
            pltpu.VMEM((groups, padded, BLOCK), jnp.float32),
            pltpu.VMEM((BLOCK // NZ, groups * padded, LANES), jnp.float32),
            pltpu.VMEM((NY, planes * LANES), jnp.float32),
            pltpu.VMEM((width // LANES, members * planes, LANES), jnp.float32),
        ],
        compiler_params=pltpu.CompilerParams(vmem_limit_bytes=KERNEL_MEMORY),
        name="finish",
    )(occupations, partial, below, above, z_table, y_table)


def column_kernel(arrived, multiplier, x_table, back_table, chunks, raw, columns, both):
    members, quarters, _, width = arrived.shape
    planes = quarters * 4
    blocks = chunks.shape[0]
    length = blocks * planes
    for member in range(members):
        for quarter in range(quarters):
            start = member * planes + quarter * 4
            raw[start : start + 4, :] = arrived[member, quarter]
    for part in range(width // LANES):
        lanes = slice(part * LANES, (part + 1) * LANES)
        total = unpacked(raw[:length, lanes])
        for band in range(1, members // blocks):
            total = total + unpacked(raw[band * length : (band + 1) * length, lanes])
        columns[:, lanes] = total
    waves = exact_product(x_table[...], columns[...]) * multiplier[...]
    field = exact_product(back_table[...], waves)
    for index, values in enumerate((columns[...], field)):
        peak = jnp.max(jnp.max(jnp.abs(values), axis=1, keepdims=True), axis=0, keepdims=True)
        lift = power_over(peak)
        for part in range(width // LANES):
            at = index * width + part * LANES
            both[:, at : at + LANES] = packed(values[:, part * LANES : (part + 1) * LANES], lift)
    for block in range(blocks):
        for quarter in range(quarters):
            start = block * planes + quarter * 4
            chunks[block, quarter] = both[start : start + 4, :]


def column_waves(arrived, multiplier, x_table, blocks):
    members, quarters, _, width = arrived.shape
    length = x_table.shape[0]
    return pl.pallas_call(
        column_kernel,
        out_shape=pltpu.VMEM((blocks, quarters, 4, 2 * width), jnp.float32),
        out_specs=pl.BlockSpec(memory_space=pltpu.VMEM),
        scratch_shapes=[
            pltpu.VMEM((members * quarters * 4, width), jnp.float32),
            pltpu.VMEM((length, width), jnp.float32),
            pltpu.VMEM((length, 2 * width), jnp.float32),
        ],
        compiler_params=pltpu.CompilerParams(vmem_limit_bytes=KERNEL_MEMORY),
        name="column_waves",
    )(arrived, multiplier, jnp.asarray(x_table), jnp.asarray(x_table.T))


def return_kernel(arrived, y_back, z_block, density, hartree, z_table, raw, along_y, along_z, result):
    members, quarters, _, width = arrived.shape
    width //= 2
    planes = quarters * 4
    groups = result.shape[1] // planes
    spread_table(z_block, z_table)
    for member in range(members):
        for quarter in range(quarters):
            start = member * planes + quarter * 4
            for part in range(2 * width // LANES):
                raw[part, start : start + 4, :] = arrived[member, quarter, :, part * LANES : (part + 1) * LANES]
    for index, out in enumerate((density, hartree)):
        for plane in range(planes):
            for part in range(width // LANES):
                block = raw[index * (width // LANES) + part, pl.ds(plane, members, stride=planes), :]
                along_y[part * members : (part + 1) * members, plane * LANES : (plane + 1) * LANES] = unpacked(block)
        waves = product(y_back[...], along_y[...])
        for plane in range(planes):
            for part in range(BLOCK // NZ):
                along_z[plane * groups : (plane + 1) * groups, part * LANES : (part + 1) * LANES] = waves[
                    part * groups : (part + 1) * groups, plane * LANES : (plane + 1) * LANES
                ]
        cells = product(along_z[...], z_table[...], 1)
        for tile in range(BLOCK // LANES):
            result[tile] = cells[:, tile * LANES : (tile + 1) * LANES]
        for group in range(groups):
            for tile in range(BLOCK // LANES):
                at = group * BLOCK + tile * LANES
                out[:, at : at + LANES] = result[tile, pl.ds(group, planes, stride=groups), :]


def return_waves(arrived, y_table, z_table, cells):
    members, quarters, _, width = arrived.shape
    planes = quarters * 4
    groups = cells // BLOCK
    plane_shape = jax.ShapeDtypeStruct((planes, cells), jnp.float32)
    return pl.pallas_call(
        return_kernel,
        out_shape=[plane_shape, plane_shape],
        scratch_shapes=[
            pltpu.VMEM((BLOCK, BLOCK // NZ * LANES), jnp.float32),
            pltpu.VMEM((width // LANES, members * planes, LANES), jnp.float32),
            pltpu.VMEM((NY, planes * LANES), jnp.float32),
            pltpu.VMEM((planes * groups, BLOCK // NZ * LANES), jnp.float32),
            pltpu.VMEM((BLOCK // LANES, planes * groups, LANES), jnp.float32),
        ],
        compiler_params=pltpu.CompilerParams(vmem_limit_bytes=KERNEL_MEMORY),
        name="return_waves",
    )(arrived, y_table, z_table)


def wave_basis(length):
    cells = np.arange(length)
    rows = []
    waves = []
    for wave in range(length // 2 + 1):
        norm = math.sqrt((1.0 if wave in (0, length / 2) else 2.0) / length)
        rows.append(norm * np.cos(2.0 * math.pi / length * (wave * cells % length)))
        waves.append(wave)
    for wave in range(1, (length + 1) // 2):
        rows.append(math.sqrt(2.0 / length) * np.sin(2.0 * math.pi / length * (wave * cells % length)))
        waves.append(wave)
    return np.asarray(rows, np.float32), (2.0 * math.pi / length * np.asarray(waves, np.float64)) ** 2


def wave_tables(members, length):
    z_basis, z_squares = wave_basis(NZ)
    y_basis, y_squares = wave_basis(NY)
    x_basis, x_squares = wave_basis(length)
    parts = BLOCK // NZ
    z_table = np.pad(z_basis.T, ((0, 0), (0, LANES - NZ)))
    rows = NY // members
    y_table = y_basis.reshape(members, rows, NY // parts, parts).transpose(1, 0, 3, 2).reshape(NY, NY)
    return z_table, y_table, x_basis, (x_squares, y_squares, z_squares)


def density_and_field(waves, tables, cells):
    bands = lax.axis_size("band")
    blocks = lax.axis_size("space")
    members, quarters, _, width = waves.shape
    z_table, y_table, x_table, (x_squares, y_squares, z_squares) = tables
    exchange = lambda chunks: lax.all_to_all(
        chunks.astype(jnp.float16), ("band", "space"), split_axis=0, concat_axis=0, tiled=True
    ).astype(jnp.float32)
    rows = NY // members
    place = (lax.axis_index("band") * blocks + lax.axis_index("space")) * rows
    squares = (
        jnp.asarray(x_squares, jnp.float32)[:, None, None]
        + lax.dynamic_slice_in_dim(jnp.asarray(y_squares, jnp.float32), place, rows)[None, :, None]
        + jnp.asarray(np.pad(z_squares, (0, LANES - NZ), constant_values=-1e9), jnp.float32)[None, None, :]
    )
    multiplier = jnp.where(
        squares > 0, 4.0 * math.pi / jnp.where(squares > 0, squares, 1.0), 0.0
    ).reshape(-1, width)
    both = column_waves(exchange(waves), multiplier, x_table, blocks)
    spread = jnp.broadcast_to(both.astype(jnp.float16)[None], (bands, *both.shape)).reshape(members, *both.shape[1:])
    return return_waves(exchange(spread), jnp.asarray(y_table.T), jnp.asarray(z_table), cells)


def in_place(x):
    return pltpu.with_memory_space_constraint(x, pltpu.VMEM)


def per_device_blocks(orbitals, potential, occupations):
    moved, potential, table = (
        pltpu.with_memory_space_constraint(x, pltpu.HBM)
        for x in (orbitals.transpose(0, 2, 1, 3), potential, plane_table())
    )
    lower, upper = rim_copies(moved)
    below = in_place(from_behind(upper, "space", 1))
    above = in_place(from_behind(lower, "space", -1))
    partial, to_lower, to_upper = first_partial(moved, potential, table)
    terms_below = in_place(from_behind(to_upper, "space", 1))
    terms_above = in_place(from_behind(to_lower, "space", -1))
    partial = second_partial(partial, below, above, moved, potential, table)
    members = lax.axis_size("band") * lax.axis_size("space")
    tables = wave_tables(members, orbitals.shape[2] * lax.axis_size("space"))
    propagated, waves = finish(
        partial, terms_below, terms_above, occupations, jnp.asarray(tables[0]), jnp.asarray(tables[1]), members
    )
    density, hartree = density_and_field(waves, tables, orbitals.shape[3])
    return (propagated.transpose(0, 2, 1, 3), density, hartree)


def per_device(orbitals, potential, occupations):
    _, count, planes, cells = orbitals.shape
    columns = NY % (lax.axis_size("space") * lax.axis_size("band"))
    if planes < 2 * REACH or planes % 4 or count != 4 or cells % CHUNK or cells % WIDE_CHUNK or PERIOD % NZ or MARGIN != REACH * NZ or columns:
        return per_device_general(orbitals, potential, occupations)
    return per_device_blocks(orbitals, potential, occupations)


def solution(mesh):
    in_specs = (P(None, "band", "space", None), P("space", None), P("band"))
    out_specs = (P(None, "band", "space", None), P("space", None), P("space", None))
    return jax.shard_map(
        per_device, mesh=mesh, in_specs=in_specs, out_specs=out_specs, check_vma=False
    )
```
